32 devices in a mesh: blk: 8 (over z, x), order: 4 (over y, core).
Axes of the slice: x: 2, y: 2, z: 4, core: 2. Of those that a mesh axis runs over, the one named last changes fastest.
Arguments:
- field: float32 [16, 512, 4096], P(None, 'blk', 'order'), may hold values from -6 to 6
- ocean_mask: int32 [512, 4096], P('blk', 'order'), may hold values from 0 to 1, as said below
- plan: int32 [512], replicated, may hold values from 0 to 384, as said below
- legendre: bfloat16 [384, 1024, 1024], P('blk', 'order'), may hold values from -0.4375 to 0.4375
Outputs:
- coefficients: float32 [1024, 16, 2, 1024], P('blk', None, None, 'order')
The draws below stay inside these ranges and needn't reach their ends.
Inputs may be any that keep to these rules, and one draw needn't show every extreme that they name: `ocean_mask`: exactly 128 cycles are all land, at the ends of the cycle order; every other cycle has an ocean point. plan is 384 exactly at the cycles that are all land, and names every slot below 384 once at the other cycles; slot p belongs to index p // 48 of blk; the cycles of one index of blk name at most 8 slots of one index, and in every draw some index of blk names exactly 8 slots of some index.
All inputs are finite; a program needn't handle non-finite values.
Results may differ from the reference program's by a relative error of at most 0.0029.
Values may be sent and summed in bfloat16 or wider, within the bound.
A program may use at most 128 MiB of HBM per device.

```python
import jax
import jax.numpy as jnp
from jax import lax

NLON = 4096
M = 1024
L = 1024
FIELDS = 16
CYCLES = 512
SLOT_DEV = 48
SLOTS = 384
N_BLK = 8
N_ORDER = 4


def wet_cycles(key):
    folded = jax.random.fold_in(key, 11)
    dry_count = CYCLES - SLOTS
    south = jax.random.randint(folded, (), 0, dry_count + 1)
    cycles = jnp.arange(CYCLES, dtype=jnp.int32)
    inside = (cycles >= south) & (cycles < CYCLES - dry_count + south)
    return inside.astype(jnp.int32)


def draw_plan(key, part):
    wet = wet_cycles(key)
    counted = jnp.cumsum(wet).astype(jnp.int32) - 1
    owner_slot = counted % N_BLK * SLOT_DEV + counted // N_BLK
    return jnp.where(wet == 1, owner_slot, SLOTS).astype(jnp.int32)


def draw_ocean_mask(key, part):
    wet = wet_cycles(key)
    levels = jax.random.randint(jax.random.fold_in(key, 12), (CYCLES, NLON), 0, 10)
    cycles = jnp.arange(CYCLES, dtype=jnp.int32)[:, None]
    longitudes = jnp.arange(NLON, dtype=jnp.int32)[None, :]
    forced = longitudes == cycles * 37 % NLON
    ocean = ((levels < 7) | forced) & (wet[:, None] == 1)
    return ocean.astype(jnp.int32)


def strengthened(drawn, own_key, source, target, shards_of, factor):
    owner, partner = [(jnp.arange(drawn.shape[dim]) // (drawn.shape[dim] // shards_of)).reshape([-1 if axis == dim else 1 for axis in range(drawn.ndim)]) for dim in (source, target)]
    chosen = jax.random.permutation(own_key, shards_of)[partner]
    strong = (owner == chosen) | (owner == (partner + shards_of // 2) % shards_of)
    return jnp.where(strong, factor * drawn, drawn)


def block_scale(stream_key, shape, cuts, least, high):
    gain = 1.0
    for position, blocks in cuts:
        steps = jax.random.uniform(jax.random.fold_in(jax.random.fold_in(stream_key, 6), position), (blocks,), jnp.float32, least / len(cuts), high / len(cuts))
        gain = gain * jnp.repeat(jnp.exp(steps), shape[position] // blocks).reshape((-1,) + (1,) * (len(shape) - 1 - position))
    return gain


def noise(key, shape, deviation, bound, shards=(), kind=jnp.bfloat16):
    result = deviation * jax.random.normal(key, shape, jnp.float32)
    if shards:
        result = result * block_scale(key, shape, shards, -0.22, 0.18)
    return jnp.clip(result, -bound, bound).astype(kind)


def gaussian_with(own_key, shape, scale, bound, shards, heavy, kind=jnp.bfloat16):
    drawn = scale * jax.random.normal(own_key, shape, jnp.float32)
    if shards:
        drawn = drawn * block_scale(own_key, shape, shards, -0.22, 0.18)
    return jnp.clip(strengthened(drawn, jax.random.fold_in(own_key, 3), *heavy), -bound, bound).astype(kind)


def setup_inputs(seed: int = 0) -> dict:
    key_list = jax.random.split(jax.random.key(seed), 5)
    field = noise(key_list[0], (FIELDS, CYCLES, NLON), 1.0, 6.0, ((1, 8), (2, 4)), jnp.float32)
    ocean_mask = draw_ocean_mask(jax.random.fold_in(key_list[4], 71), 0)
    plan = draw_plan(jax.random.fold_in(key_list[4], 71), 0)
    legendre = gaussian_with(key_list[3], (SLOTS, M, L), SLOTS ** -0.5, 0.4375, ((0, 8), (1, 4)), (0, 2, 8, 2.0))
    return dict(field=field, ocean_mask=ocean_mask, plan=plan, legendre=legendre)


def reference(field, ocean_mask, plan, legendre):
    masked = field * ocean_mask.astype(jnp.float32)[None]
    holder = jnp.zeros((FIELDS, SLOTS + 1, NLON), jnp.float32)
    packed = holder.at[:, plan.astype(jnp.int32), :].set(masked)[:, :SLOTS]
    transform = jnp.fft.rfft(packed, axis=2)[:, :, :M] / jnp.sqrt(jnp.float32(NLON))
    spectrum = jnp.stack([jnp.real(transform), jnp.imag(transform)], axis=2).astype(jnp.float32).astype(jnp.bfloat16)
    width = M // N_ORDER

    def one_block(block_index):
        first = (block_index * width).astype(jnp.int32)
        table = lax.dynamic_slice_in_dim(legendre, first, width, 1).astype(jnp.float32)
        values = lax.dynamic_slice_in_dim(spectrum, first, width, 3).astype(jnp.float32)
        return jnp.einsum('pml,fpcm->lfcm', table, values)
    blocks = lax.map(one_block, jnp.arange(N_ORDER, dtype=jnp.int32))
    moved = jnp.moveaxis(blocks, 0, 3)
    return moved.reshape(L, FIELDS, 2, M)
```

```python
import functools
import math

import jax
import jax.numpy as jnp
import numpy as np
from jax import lax
from jax.experimental import pallas as pl
from jax.experimental.pallas import tpu as pltpu
from jax.sharding import PartitionSpec as P

NLON = 4096
M = 1024
MESH = pl.DeviceIdType.MESH
F32, BF16 = jnp.float32, jnp.bfloat16

LINE, PAIR = 4, 2
CHUNK = 2
BASE = 32


def table_of(lon_local, orders):
    coarse = np.arange(lon_local // BASE)[:, None] * BASE
    fine = np.arange(BASE)[:, None]
    m = np.arange(M)[None, :]

    def parts(n, scale):
        angle = (n * m % NLON) * (2.0 * math.pi / NLON)
        return [np.cos(angle) * scale, np.sin(angle) * scale]

    both = parts(coarse, 1.0) + parts(fine, 1.0 / math.sqrt(NLON))
    owners = M // orders
    stacked = np.stack([t.reshape(BASE, owners, orders) for t in both])
    return stacked.transpose(2, 0, 1, 3).astype(np.float32)


def plan_maps(plan, cycle_dev, slot_dev, orders_tile):
    n_blk = lax.axis_size("blk")
    own_index = lax.axis_index("blk")
    cap = (cycle_dev + n_blk - 1) // n_blk
    grid = plan.reshape(n_blk, cycle_dev)
    owner = grid // slot_dev
    positions = jnp.arange(cycle_dev, dtype=jnp.int32)
    earlier = positions[None, :] < positions[:, None]
    same_owner = owner[:, :, None] == owner[:, None, :]
    rank = jnp.sum(same_owner & earlier[None], axis=2, dtype=jnp.int32)
    send_pos = owner * cap + rank
    local_pos = lax.dynamic_index_in_dim(send_pos, own_index, 0, keepdims=False)
    source_pos = (jnp.arange(n_blk, dtype=jnp.int32)[:, None] * cap + rank).reshape(-1)
    lanes = jnp.arange(slot_dev * orders_tile, dtype=jnp.int32) // orders_tile
    wanted = own_index * slot_dev + lanes
    hit = plan.reshape(-1)[:, None] == wanted[None, :]
    received = jnp.sum(jnp.where(hit, source_pos[:, None], 0), axis=0, dtype=jnp.int32)
    return jnp.tile(local_pos, CHUNK)[None, :], received[None, :]


def fused_kernel(
    dims,
    field, mask, legendre, table, send_lanes, recv_lanes,
    out, far_field,
    leg, spread, own_part, xs, xr, zr, wh, wl, near, far, mask_near, mask_far, parts,
    y_own, y_send, y_recv, a_send, a_recv, pick, pack, stage, tabs,
    leg_sem, near_sem, far_sem, mask_sem, tab_sem, out_sem,
    pf_send, pf_recv, pm_send, pm_recv, ys_sem, yr_sem, as_sem, ar_sem,
    xs_sem, xr_sem, zs_sem, zr_sem,
):
    n, groups, tile, m_dev, l_dev, cyc, lon, slot_dev, cap = dims
    rows = CHUNK * cyc
    n_blk = LINE * PAIR
    b = lax.axis_index("blk")
    o = lax.axis_index("order")
    z, x = b // PAIR, b % PAIR
    side = z // 2
    odd = z % 2
    is_end = 1 - (odd + side - 2 * odd * side)
    far_end = (LINE - 1) * (1 - side)
    far_inner = 2 - side
    mate = 2 * side + 1 - odd
    dest = [
        is_end * far_end + (1 - is_end) * mate,
        is_end * far_inner + (1 - is_end) * far_end,
        is_end * mate + (1 - is_end) * far_inner,
        z,
    ]
    x_peer = b + 1 - 2 * x
    y_peer = (o + 2) % 4
    c_peer = o + 1 - 2 * (o % 2)

    def remote(src, dst, send, recv, blk, order):
        return pltpu.make_async_remote_copy(
            src_ref=src, dst_ref=dst, send_sem=send, recv_sem=recv,
            device_id=(blk, order), device_id_type=MESH,
        )

    def leg_copy(half, j):
        block = dest[j] * PAIR + (x if half == 0 else 1 - x)
        lanes = pl.ds(pl.multiple_of(block * l_dev, l_dev), l_dev)
        return pltpu.make_async_copy(
            legendre.at[:, :, lanes],
            leg.at[half, :, :, pl.ds(j * l_dev, l_dev)],
            leg_sem.at[half, j],
        )

    def near_copy(h):
        return pltpu.make_async_copy(
            field.at[pl.ds(h * CHUNK, CHUNK)], near.at[h % 2], near_sem.at[h % 2]
        )

    def far_copy(h):
        return pltpu.make_async_copy(
            far_field.at[pl.ds(h * CHUNK, CHUNK)], far.at[h % 2], far_sem.at[h % 2]
        )

    def push_field(h):
        fields = pl.ds(h * CHUNK, CHUNK)
        return remote(
            field.at[fields], far_field.at[fields], pf_send.at[h], pf_recv.at[h], b, c_peer
        )

    tab_own = pltpu.make_async_copy(table.at[o], tabs.at[0], tab_sem.at[0])
    tab_other = pltpu.make_async_copy(table.at[y_peer], tabs.at[1], tab_sem.at[1])
    tab_own.start()
    tab_other.start()
    mask_own = pltpu.make_async_copy(mask, mask_near, mask_sem)
    mask_own.start()
    near_copy(0).start()

    barrier = pltpu.get_barrier_semaphore()
    for k in range(1, n_blk):
        pl.semaphore_signal(barrier, inc=1, device_id=((b + k) % n_blk, o), device_id_type=MESH)
    pl.semaphore_signal(barrier, inc=1, device_id=(b, y_peer), device_id_type=MESH)
    pl.semaphore_signal(barrier, inc=1, device_id=(b, c_peer), device_id_type=MESH)
    pl.semaphore_wait(barrier, n_blk + 1)

    push_mask = remote(mask, mask_far, pm_send, pm_recv, b, c_peer)
    push_mask.start()

    @pl.loop(0, n)
    def _(h):
        push_field(h).start()

    for half in (1, 0):
        for j in range(LINE):
            leg_copy(half, j).start()

    def iota(shape, axis):
        return lax.broadcasted_iota(jnp.int32, shape, axis)

    r = iota((rows, rows), 0)
    lane = iota((rows, rows), 1)
    per = CHUNK * cap
    position = r // per * cap + r % cap
    hit = (position == send_lanes[...]) & (r % per // cap == lane // cyc)
    pack[...] = jnp.where(hit, 1.0, 0.0).astype(BF16)
    r = iota((rows, slot_dev * tile), 0)
    position = r // per * cap + r % cap
    for f in range(CHUNK):
        hit = (position == recv_lanes[...]) & (r % per // cap == f)
        pick[f] = jnp.where(hit, 1.0, 0.0).astype(BF16)

    tab_own.wait()
    tab_other.wait()
    for side_of in range(2):

        @pl.loop(0, lon // BASE)
        def _(a):
            ca = tabs[side_of, 0, pl.ds(a, 1), :]
            sa = tabs[side_of, 1, pl.ds(a, 1), :]
            cb = tabs[side_of, 2]
            sb = tabs[side_of, 3]
            at = pl.ds(pl.multiple_of(a * BASE, BASE), BASE)
            for c, value in enumerate((ca * cb - sa * sb, -(sa * cb + ca * sb))):
                high = value.astype(BF16)
                wh[side_of, at, pl.ds(c * m_dev, m_dev)] = high
                rest = value - high.astype(F32)
                wl[side_of, at, pl.ds(c * m_dev, m_dev)] = rest.astype(BF16)

    mask_own.wait()
    push_mask.wait_recv()
    push_field(0).wait_recv()
    far_copy(0).start()

    def turn(index):
        quarter = (index * iota((1, m_dev), 1)) % 4
        real = jnp.where(quarter == 0, 1.0, jnp.where(quarter == 2, -1.0, 0.0))
        imag = jnp.where(quarter == 3, 1.0, jnp.where(quarter == 1, -1.0, 0.0))
        return real, imag

    def y_copy(h):
        return remote(y_send.at[h % 2], y_recv.at[h], ys_sem.at[h % 2], yr_sem.at[h], b, y_peer)

    def transform(h):
        near_copy(h).wait()
        far_copy(h).wait()

        @pl.when(h + 1 < n)
        def _():
            near_copy(h + 1).start()
            push_field(h + 1).wait_recv()
            far_copy(h + 1).start()

        @pl.when(h >= 2)
        def _():
            y_copy(h - 2).wait_send()

        for i, (data, wet) in enumerate(((near, mask_near), (far, mask_far))):
            value = (data[h % 2] * wet[...].astype(F32)[None]).reshape(rows, lon)
            high = value.astype(BF16)
            parts[pl.ds(i * rows, rows), :] = high
            rest = value - high.astype(F32)
            parts[pl.ds((2 + i) * rows, rows), :] = rest.astype(BF16)
        near_r, near_i = turn(o)
        far_r, far_i = turn(c_peer)
        for side_of in (1, 0):
            both = jnp.dot(parts[...], wh[side_of], preferred_element_type=F32)
            total = both[: 2 * rows] + both[2 * rows :]
            total += jnp.dot(
                parts[pl.ds(0, 2 * rows), :], wl[side_of], preferred_element_type=F32
            )
            nr, ni = total[:rows, :m_dev], total[:rows, m_dev:]
            fr, fi = total[rows:, :m_dev], total[rows:, m_dev:]
            real = near_r * nr - near_i * ni + far_r * fr - far_i * fi
            imag = near_r * ni + near_i * nr + far_r * fi + far_i * fr
            target = y_send if side_of else y_own
            target[h % 2, :, pl.ds(0, m_dev)] = real
            target[h % 2, :, pl.ds(m_dev, m_dev)] = imag
            if side_of:
                y_copy(h).start()

    def a_copy(h, k):
        to = (b + k) % n_blk
        return remote(
            a_send.at[h, to], a_recv.at[h, b], as_sem.at[h, k - 1], ar_sem.at[h, k - 1], to, o
        )

    def exchange(h):
        y_copy(h).wait_recv()
        spectrum = (y_own[h % 2] + y_recv[h]).astype(BF16)
        packed = jnp.dot(pack[...], spectrum, preferred_element_type=F32).astype(BF16)
        a_send[h] = packed.reshape(n_blk, per, 2 * m_dev)
        a_recv[h, b] = a_send[h, b]
        for k in range(1, n_blk):
            a_copy(h, k).start()

    diagonal = (iota((1, tile, slot_dev * tile), 1)) == (iota((1, tile, slot_dev * tile), 2) % tile)

    def spread_out(h):
        for k in range(1, n_blk):
            a_copy(h, k).wait_recv()
        got = a_recv[h].reshape(rows, 2 * m_dev)
        for c in range(2):
            for f in range(CHUNK):
                value = lax.dot_general(
                    got[:, c * m_dev : (c + 1) * m_dev], pick[f],
                    (((0,), (0,)), ((), ())), preferred_element_type=F32,
                )
                value = value.reshape(groups, tile, slot_dev * tile)
                spread[:, pl.ds((f * 2 + c) * tile, tile), :] = jnp.where(
                    diagonal, value, 0.0
                ).astype(BF16)

    def x_copy(h, j):
        return remote(
            xs.at[h % 2, j], xr.at[h % 5, j], xs_sem.at[h % 2, j], xr_sem.at[h, j], x_peer, o
        )

    def product(g, half):
        at = pl.ds(pl.multiple_of(g * tile, tile), tile)
        table_part = leg[half, :, at, :].reshape(slot_dev * tile, LINE * l_dev)
        return at, jnp.dot(spread[g], table_part, preferred_element_type=F32)

    def products(h):
        @pl.when(h == 0)
        def _():
            for j in range(LINE):
                leg_copy(1, j).wait()

        @pl.when(h >= 2)
        def _():
            for j in range(LINE):
                x_copy(h - 2, j).wait_send()

        @pl.loop(0, groups)
        def _(g):
            at, value = product(g, 1)
            for j in range(LINE):
                piece = value[:, j * l_dev : (j + 1) * l_dev].reshape(2 * CHUNK, tile, l_dev)
                xs[h % 2, j, :, at, :] = piece.astype(BF16)

        for j in range(LINE):
            x_copy(h, j).start()

        @pl.when(h == 0)
        def _():
            for j in range(LINE):
                leg_copy(0, j).wait()

        @pl.loop(0, groups)
        def _(g):
            at, value = product(g, 0)
            for j in range(LINE):
                piece = value[:, j * l_dev : (j + 1) * l_dev].reshape(2 * CHUNK, tile, l_dev)
                own_part[h % 3, j, :, at, :] = piece

    def z_copy(h, j, to_z, slot):
        return remote(
            xr.at[h % 5, j], zr.at[h % 4, slot], zs_sem.at[h, j], zr_sem.at[h, slot],
            to_z * PAIR + x, o,
        )

    def end_copy(h, j):
        return z_copy(h, j, mate, j)

    def inner_copy(h, j):
        return z_copy(h, j, (mate, far_end, far_inner)[j], (0, 1, 3)[j])

    def first_sums(h):
        for j in range(LINE):
            x_copy(h, j).wait_recv()
            value = own_part[h % 3, j] + xr[h % 5, j].astype(F32)
            if j == LINE - 1:
                own_part[h % 3, j] = value
                continue

            @pl.when(is_end == 1)
            def _():
                xr[h % 5, j] = value.astype(BF16)
                end_copy(h, j).start()

            @pl.when(is_end == 0)
            def _():
                if j == 0:
                    xr[h % 5, j] = value.astype(BF16)
                    inner_copy(h, j).start()
                else:
                    own_part[h % 3, j] = value

    def second_sums(h):
        @pl.when(is_end == 0)
        def _():
            for j in (1, 2):
                end_copy(h, j - 1).wait_recv()
                value = own_part[h % 3, j] + zr[h % 4, j - 1].astype(F32)
                xr[h % 5, j] = value.astype(BF16)
                inner_copy(h, j).start()

    def out_copy(h):
        return pltpu.make_async_copy(stage.at[h % 2], out.at[h], out_sem.at[h % 2])

    def last_sums(h):
        @pl.when(h >= 2)
        def _():
            out_copy(h - 2).wait()

        @pl.when(is_end == 1)
        def _():
            inner_copy(h, 0).wait_recv()
            inner_copy(h, 1).wait_recv()
            stage[h % 2] = own_part[h % 3, 3] + zr[h % 4, 0].astype(F32) + zr[h % 4, 1].astype(F32)
            for j in range(3):
                end_copy(h, j).wait_send()

        @pl.when(is_end == 0)
        def _():
            end_copy(h, 2).wait_recv()
            inner_copy(h, 2).wait_recv()
            stage[h % 2] = own_part[h % 3, 3] + zr[h % 4, 2].astype(F32) + zr[h % 4, 3].astype(F32)
            for j in range(3):
                inner_copy(h, j).wait_send()

        out_copy(h).start()

    @pl.loop(0, n + 5)
    def _(t):
        def when(step, delay):
            @pl.when((t >= delay) & (t < n + delay))
            def _():
                step(t - delay)

        when(last_sums, 5)
        when(transform, 0)
        when(exchange, 1)
        when(spread_out, 2)
        when(products, 2)
        when(second_sums, 4)
        when(first_sums, 3)

    push_mask.wait_send()

    @pl.loop(0, n)
    def _(h):
        push_field(h).wait_send()
        for k in range(1, n_blk):
            a_copy(h, k).wait_send()

    for h in (n - 2, n - 1):
        y_copy(h).wait_send()
        out_copy(h).wait()
        for j in range(LINE):
            x_copy(h, j).wait_send()


def fused_body(field, ocean_mask, plan, legendre):
    fields, cyc, lon = field.shape
    slot_dev, m_dev, degrees = legendre.shape
    n_blk = LINE * PAIR
    l_dev = degrees // n_blk
    tile = 16
    groups = m_dev // tile
    n = fields // CHUNK
    rows = CHUNK * cyc
    cap = (cyc + n_blk - 1) // n_blk
    per = CHUNK * cap
    send_lanes, recv_lanes = plan_maps(plan, cyc, slot_dev, tile)
    table = jnp.asarray(table_of(lon, m_dev))
    piece = (2 * CHUNK, m_dev, l_dev)
    dma = pltpu.SemaphoreType.DMA
    any_spec = pl.BlockSpec(memory_space=pl.ANY)
    vmem_spec = pl.BlockSpec(memory_space=pltpu.VMEM)
    scratch = [
        pltpu.VMEM((2, slot_dev, m_dev, LINE * l_dev), BF16),
        pltpu.VMEM((groups, 2 * CHUNK * tile, slot_dev * tile), BF16),
        pltpu.VMEM((3, LINE) + piece, F32),
        pltpu.VMEM((2, LINE) + piece, BF16),
        pltpu.VMEM((5, LINE) + piece, BF16),
        pltpu.VMEM((4, 4) + piece, BF16),
        pltpu.VMEM((2, lon, 2 * m_dev), BF16),
        pltpu.VMEM((2, lon, 2 * m_dev), BF16),
        pltpu.VMEM((2, CHUNK, cyc, lon), F32),
        pltpu.VMEM((2, CHUNK, cyc, lon), F32),
        pltpu.VMEM((cyc, lon), jnp.int32),
        pltpu.VMEM((cyc, lon), jnp.int32),
        pltpu.VMEM((4 * rows, lon), BF16),
        pltpu.VMEM((2, rows, 2 * m_dev), F32),
        pltpu.VMEM((2, rows, 2 * m_dev), F32),
        pltpu.VMEM((n, rows, 2 * m_dev), F32),
        pltpu.VMEM((n, n_blk, per, 2 * m_dev), BF16),
        pltpu.VMEM((n, n_blk, per, 2 * m_dev), BF16),
        pltpu.VMEM((CHUNK, rows, slot_dev * tile), BF16),
        pltpu.VMEM((rows, rows), BF16),
        pltpu.VMEM((2,) + piece, F32),
        pltpu.VMEM((2, 4, BASE, m_dev), F32),
        dma((2, LINE)),
        dma((2,)),
        dma((2,)),
        dma,
        dma((2,)),
        dma((2,)),
        dma((n,)), dma((n,)),
        dma, dma,
        dma((2,)), dma((n,)),
        dma((n, n_blk - 1)), dma((n, n_blk - 1)),
        dma((2, LINE)), dma((n, LINE)),
        dma((n, 3)), dma((n, 4)),
    ]
    dims = (n, groups, tile, m_dev, l_dev, cyc, lon, slot_dev, cap)
    sums, _ = pl.pallas_call(
        functools.partial(fused_kernel, dims),
        out_shape=[
            jax.ShapeDtypeStruct((n,) + piece, F32),
            jax.ShapeDtypeStruct(field.shape, F32),
        ],
        in_specs=[any_spec] * 4 + [vmem_spec] * 2,
        out_specs=[any_spec] * 2,
        scratch_shapes=scratch,
        compiler_params=pltpu.CompilerParams(
            collective_id=0, has_side_effects=True, vmem_limit_bytes=66 * 1000 * 1000
        ),
        name="analysis",
    )(field, ocean_mask, legendre, table, send_lanes, recv_lanes)
    sums = sums.reshape(fields, 2, m_dev, l_dev)
    return jnp.transpose(sums, (3, 0, 1, 2))


def fits(mesh, field, legendre):
    shape = dict(mesh.shape)
    n_blk, n_order = shape["blk"], shape["order"]
    cyc, lon = field.shape[1] // n_blk, field.shape[2] // n_order
    slots, m_dev = legendre.shape[0] // n_blk, legendre.shape[1] // n_order
    return (
        n_blk == LINE * PAIR
        and n_order == 4
        and field.shape[0] % CHUNK == 0
        and field.shape[0] // CHUNK >= 5
        and lon == BASE * BASE
        and NLON == 4 * lon
        and m_dev % 128 == 0
        and legendre.shape[2] == n_blk * 128
        and cyc % n_blk == 0
        and slots % 8 == 0
    )


def twiddle(first, count):
    longitudes = first + jnp.arange(count, dtype=jnp.int32)
    orders = jnp.arange(M, dtype=jnp.int32)
    product = longitudes[:, None] * orders[None, :] % NLON
    angle = product.astype(jnp.float32) * (2.0 * math.pi / NLON)
    scale = 1.0 / math.sqrt(NLON)
    return jnp.stack([jnp.cos(angle) * scale, -jnp.sin(angle) * scale], axis=1)


def transform(values, table):
    return jnp.einsum("frn,ncm->frcm", values, table, precision=lax.Precision.HIGHEST)


def pack_cycles(masked, plan, slot_dev):
    n_blk = lax.axis_size("blk")
    own_index = lax.axis_index("blk")
    cycle_dev = masked.shape[1]
    cap = (cycle_dev + n_blk - 1) // n_blk
    grid = plan.reshape(n_blk, cycle_dev)
    owner = grid // slot_dev
    positions = jnp.arange(cycle_dev, dtype=jnp.int32)
    earlier = positions[None, :] < positions[:, None]
    same_owner = owner[:, :, None] == owner[:, None, :]
    rank = jnp.sum(same_owner & earlier[None], axis=2, dtype=jnp.int32)
    send_pos = owner * cap + rank
    local_pos = lax.dynamic_index_in_dim(send_pos, own_index, 0, keepdims=False)
    buffer_ids = jnp.arange(n_blk * cap, dtype=jnp.int32)
    send_onehot = (buffer_ids[:, None] == local_pos[None, :]).astype(jnp.float32)
    outgoing = jnp.einsum("qr,frn->fqn", send_onehot, masked, precision=lax.Precision.HIGHEST)
    arrived = lax.all_to_all(outgoing, "blk", split_axis=1, concat_axis=1, tiled=True)
    source_pos = (jnp.arange(n_blk, dtype=jnp.int32)[:, None] * cap + rank).reshape(-1)
    mine = (owner == own_index).reshape(-1)
    slot_local = (grid % slot_dev).reshape(-1)
    slot_ids = jnp.arange(slot_dev, dtype=jnp.int32)
    slot_onehot = ((slot_local[None, :] == slot_ids[:, None]) & mine[None, :]).astype(jnp.float32)
    source_onehot = (source_pos[:, None] == buffer_ids[None, :]).astype(jnp.float32)
    receive_map = jnp.dot(slot_onehot, source_onehot, precision=lax.Precision.HIGHEST)
    return jnp.einsum("pq,fqn->fpn", receive_map, arrived, precision=lax.Precision.HIGHEST)


def degree_sums(legendre, spectrum):
    n_blk = lax.axis_size("blk")
    own_index = lax.axis_index("blk")
    pairs = n_blk // 2
    degree_dev = legendre.shape[2] // n_blk
    own_pair, own_side = own_index // 2, own_index % 2
    swap = [(i, i + 1 - 2 * (i % 2)) for i in range(n_blk)]

    def terms_for(target):
        table = lax.dynamic_slice_in_dim(legendre, target * degree_dev, degree_dev, 2)
        return jnp.einsum("pml,fpcm->lfcm", table, spectrum, preferred_element_type=jnp.float32)

    def pair_sum(step):
        base = (own_pair + step) % pairs * 2
        given = terms_for(base + 1 - own_side).astype(jnp.bfloat16)
        taken = lax.ppermute(given, "blk", swap)
        return terms_for(base + own_side) + taken.astype(jnp.float32)

    steps = sorted(range(1, pairs), key=lambda step: abs(2 * step - pairs))
    arrived = []
    for step in steps:
        shift = [(i, (i + 2 * step) % n_blk) for i in range(n_blk)]
        arrived.append(lax.ppermute(pair_sum(step).astype(jnp.bfloat16), "blk", shift))
    total = pair_sum(0)
    for piece in arrived:
        total = total + piece.astype(jnp.float32)
    return total


def body(field, ocean_mask, plan, legendre):
    lon_local = field.shape[2]
    slot_dev = legendre.shape[0]
    masked = field * ocean_mask.astype(jnp.float32)[None]
    packed = pack_cycles(masked, plan, slot_dev)
    first = lax.axis_index("order") * lon_local
    terms = transform(packed, twiddle(first, lon_local))
    spectrum = lax.psum_scatter(terms, "order", scatter_dimension=3, tiled=True).astype(
        jnp.bfloat16
    )
    coefficients = degree_sums(legendre, spectrum)
    return coefficients


def solution(mesh):
    placed = (P(None, "blk", "order"), P("blk", "order"), P(), P("blk", "order", None))

    def run(field, ocean_mask, plan, legendre):
        chosen = fused_body if fits(mesh, field, legendre) else body
        mapped = jax.shard_map(
            chosen, mesh=mesh, in_specs=placed, out_specs=P("blk", None, None, "order"),
            check_vma=False,
        )
        return mapped(field, ocean_mask, plan, legendre)

    return run
```

```python
import functools
import math

import jax
import jax.numpy as jnp
import numpy as np
from jax import lax
from jax.experimental import pallas as pl
from jax.experimental.pallas import tpu as pltpu
from jax.sharding import PartitionSpec as P

NLON = 4096
M = 1024
MESH = pl.DeviceIdType.MESH
F32, BF16 = jnp.float32, jnp.bfloat16

LINE, PAIR = 4, 2
CHUNK = 2
BASE = 32


def table_of(lon_local, orders):
    coarse = np.arange(lon_local // BASE)[:, None] * BASE
    fine = np.arange(BASE)[:, None]
    m = np.arange(M)[None, :]

    def parts(n, scale):
        angle = (n * m % NLON) * (2.0 * math.pi / NLON)
        return [np.cos(angle) * scale, np.sin(angle) * scale]

    both = parts(coarse, 1.0) + parts(fine, 1.0 / math.sqrt(NLON))
    owners = M // orders
    stacked = np.stack([t.reshape(BASE, owners, orders) for t in both])
    return stacked.transpose(2, 0, 1, 3).astype(np.float32)


def fused_kernel(
    dims,
    field, mask, legendre, table, plan,
    out, far_field,
    leg, spread, own_part, far_part, xs, xr, zr, zbs, zbr, xbs, xbr, wh, wl, near, far, mask_near, mask_far, parts,
    y_own, y_send, y_recv, a_send, a_recv, pick, pack, stage, tabs,
    leg_sem, near_sem, far_sem, mask_sem, tab_sem, out_sem,
    pf_send, pf_recv, pm_send, pm_recv, ys_sem, yr_sem, as_sem, ar_sem,
    xs_sem, xr_sem, zs_sem, zr_sem, zbs_sem, zbr_sem, xbs_sem, xbr_sem,
):
    n, groups, x_groups, tile, m_dev, l_dev, cyc, lon, slot_dev, cap = dims
    m_x = x_groups * tile
    rows = CHUNK * cyc
    n_blk = LINE * PAIR
    b = lax.axis_index("blk")
    o = lax.axis_index("order")
    z, x = b // PAIR, b % PAIR
    side = z // 2
    odd = z % 2
    is_end = 1 - (odd + side - 2 * odd * side)
    far_end = (LINE - 1) * (1 - side)
    far_inner = 2 - side
    mate = 2 * side + 1 - odd
    dest = [
        is_end * far_end + (1 - is_end) * mate,
        is_end * far_inner + (1 - is_end) * far_end,
        is_end * mate + (1 - is_end) * far_inner,
        z,
    ]
    x_peer = b + 1 - 2 * x
    y_peer = (o + 2) % 4
    c_peer = o + 1 - 2 * (o % 2)

    def remote(src, dst, send, recv, blk, order):
        return pltpu.make_async_remote_copy(
            src_ref=src, dst_ref=dst, send_sem=send, recv_sem=recv,
            device_id=(blk, order), device_id_type=MESH,
        )

    def leg_copy(half, j):
        block = dest[j] * PAIR + (x if half == 0 else 1 - x)
        lanes = pl.ds(pl.multiple_of(block * l_dev, l_dev), l_dev)
        return pltpu.make_async_copy(
            legendre.at[:, :, lanes],
            leg.at[half, :, :, pl.ds(j * l_dev, l_dev)],
            leg_sem.at[half, j],
        )

    def near_copy(h):
        return pltpu.make_async_copy(
            field.at[pl.ds(h * CHUNK, CHUNK)], near.at[h % 2], near_sem.at[h % 2]
        )

    def far_copy(h):
        return pltpu.make_async_copy(
            far_field.at[pl.ds(h * CHUNK, CHUNK)], far.at[h % 2], far_sem.at[h % 2]
        )

    def push_field(h):
        fields = pl.ds(h * CHUNK, CHUNK)
        return remote(
            field.at[fields], far_field.at[fields], pf_send.at[h], pf_recv.at[h], b, c_peer
        )

    def push_first():
        return remote(
            field.at[pl.ds(0, CHUNK)], far.at[0], pf_send.at[0], pf_recv.at[0], b, c_peer
        )

    tab_own = pltpu.make_async_copy(table.at[o], tabs.at[0], tab_sem.at[0])
    tab_other = pltpu.make_async_copy(table.at[y_peer], tabs.at[1], tab_sem.at[1])
    tab_own.start()
    tab_other.start()
    mask_own = pltpu.make_async_copy(mask, mask_near, mask_sem)
    mask_own.start()
    near_copy(0).start()

    barrier = pltpu.get_barrier_semaphore()
    for k in range(1, n_blk):
        pl.semaphore_signal(barrier, inc=1, device_id=((b + k) % n_blk, o), device_id_type=MESH)
    pl.semaphore_signal(barrier, inc=1, device_id=(b, y_peer), device_id_type=MESH)
    pl.semaphore_signal(barrier, inc=1, device_id=(b, c_peer), device_id_type=MESH)

    def iota(shape, axis):
        return lax.broadcasted_iota(jnp.int32, shape, axis)

    wanted = (b * slot_dev + iota((1, slot_dev * tile), 1) // tile).astype(F32)
    row_id, col_id = iota((cyc, cyc), 0), iota((cyc, cyc), 1)
    send_at = jnp.zeros((1, cyc), F32)
    source = jnp.zeros((cyc, slot_dev * tile), F32)
    for block in range(n_blk):
        across = plan[pl.ds(block, 1), :].astype(F32)
        down = jnp.sum(jnp.where(row_id == col_id, across, 0.0), axis=1, keepdims=True)
        owner_across = jnp.floor((across + 0.5) * (1.0 / slot_dev))
        owner_down = jnp.floor((down + 0.5) * (1.0 / slot_dev))
        same = owner_down == owner_across
        rank_across = jnp.sum(
            jnp.where(same & (row_id < col_id), 1.0, 0.0), axis=0, keepdims=True
        )
        rank_down = jnp.sum(
            jnp.where(same & (col_id < row_id), 1.0, 0.0), axis=1, keepdims=True
        )
        here = jnp.where(b == block, 1.0, 0.0)
        send_at += here * (owner_across * cap + rank_across)
        source += jnp.where(down == wanted, block * cap + rank_down, 0.0)
    source = jnp.sum(source, axis=0, keepdims=True)
    per = CHUNK * cap
    r = iota((rows, cyc), 0)
    position = (r // per * cap + r % cap).astype(F32)
    for f in range(CHUNK):
        hit = (position == send_at) & (r % per // cap == f)
        pack[:, pl.ds(f * cyc, cyc)] = jnp.where(hit, 1.0, 0.0).astype(BF16)
    r = iota((rows, slot_dev * tile), 0)
    position = (r // per * cap + r % cap).astype(F32)
    for f in range(CHUNK):
        hit = (position == source) & (r % per // cap == f)
        pick[f] = jnp.where(hit, 1.0, 0.0).astype(BF16)

    pl.semaphore_wait(barrier, n_blk + 1)

    push_mask = remote(mask, mask_far, pm_send, pm_recv, b, c_peer)
    push_mask.start()
    push_first().start()

    @pl.loop(1, n)
    def _(h):
        push_field(h).start()

    tab_own.wait()
    tab_other.wait()
    for side_of in range(2):

        @pl.loop(0, lon // BASE)
        def _(a):
            ca = tabs[side_of, 0, pl.ds(a, 1), :]
            sa = tabs[side_of, 1, pl.ds(a, 1), :]
            cb = tabs[side_of, 2]
            sb = tabs[side_of, 3]
            at = pl.ds(pl.multiple_of(a * BASE, BASE), BASE)
            for c, value in enumerate((ca * cb - sa * sb, -(sa * cb + ca * sb))):
                high = value.astype(BF16)
                wh[side_of, at, pl.ds(c * m_dev, m_dev)] = high
                rest = value - high.astype(F32)
                wl[side_of, at, pl.ds(c * m_dev, m_dev)] = rest.astype(BF16)

    mask_own.wait()
    push_mask.wait_recv()

    def turn(index):
        quarter = (index * iota((1, m_dev), 1)) % 4
        real = jnp.where(quarter == 0, 1.0, jnp.where(quarter == 2, -1.0, 0.0))
        imag = jnp.where(quarter == 3, 1.0, jnp.where(quarter == 1, -1.0, 0.0))
        return real, imag

    def y_copy(h):
        return remote(y_send.at[h % 2], y_recv.at[h], ys_sem.at[h % 2], yr_sem.at[h], b, y_peer)

    def transform(h):
        near_copy(h).wait()

        @pl.when(h == 0)
        def _():
            push_first().wait_recv()
            for half in (1, 0):
                for j in range(LINE):
                    leg_copy(half, j).start()

        @pl.when(h > 0)
        def _():
            far_copy(h).wait()

        @pl.when(h + 1 < n)
        def _():
            near_copy(h + 1).start()
            push_field(h + 1).wait_recv()
            far_copy(h + 1).start()

        @pl.when(h >= 2)
        def _():
            y_copy(h - 2).wait_send()

        for i, (data, wet) in enumerate(((near, mask_near), (far, mask_far))):
            value = (data[h % 2] * wet[...].astype(F32)[None]).reshape(rows, lon)
            high = value.astype(BF16)
            parts[pl.ds(i * rows, rows), :] = high
            rest = value - high.astype(F32)
            parts[pl.ds((2 + i) * rows, rows), :] = rest.astype(BF16)
        near_r, near_i = turn(o)
        far_r, far_i = turn(c_peer)
        for side_of in (1, 0):
            both = jnp.dot(parts[...], wh[side_of], preferred_element_type=F32)
            total = both[: 2 * rows] + both[2 * rows :]
            total += jnp.dot(
                parts[pl.ds(0, 2 * rows), :], wl[side_of], preferred_element_type=F32
            )
            nr, ni = total[:rows, :m_dev], total[:rows, m_dev:]
            fr, fi = total[rows:, :m_dev], total[rows:, m_dev:]
            real = near_r * nr - near_i * ni + far_r * fr - far_i * fi
            imag = near_r * ni + near_i * nr + far_r * fi + far_i * fr
            target = y_send if side_of else y_own
            target[h % 2, :, pl.ds(0, m_dev)] = real
            target[h % 2, :, pl.ds(m_dev, m_dev)] = imag
            if side_of:
                y_copy(h).start()

    def a_copy(h, k):
        to = (b + k) % n_blk
        return remote(
            a_send.at[h, to], a_recv.at[h, b], as_sem.at[h, k - 1], ar_sem.at[h, k - 1], to, o
        )

    def exchange(h):
        y_copy(h).wait_recv()
        spectrum = (y_own[h % 2] + y_recv[h]).astype(BF16)
        packed = jnp.dot(pack[...], spectrum, preferred_element_type=F32).astype(BF16)
        a_send[h] = packed.reshape(n_blk, per, 2 * m_dev)
        a_recv[h, b] = a_send[h, b]
        for k in range(1, n_blk):
            a_copy(h, k).start()

    diagonal = (iota((1, tile, slot_dev * tile), 1)) == (iota((1, tile, slot_dev * tile), 2) % tile)

    def spread_out(h):
        for k in range(1, n_blk):
            a_copy(h, k).wait_recv()
        got = a_recv[h].reshape(rows, 2 * m_dev)
        for c in range(2):
            for f in range(CHUNK):
                value = lax.dot_general(
                    got[:, c * m_dev : (c + 1) * m_dev], pick[f],
                    (((0,), (0,)), ((), ())), preferred_element_type=F32,
                )
                value = value.reshape(groups, tile, slot_dev * tile)
                spread[:, pl.ds((f * 2 + c) * tile, tile), :] = jnp.where(
                    diagonal, value, 0.0
                ).astype(BF16)

    def x_copy(h, j):
        return remote(
            xs.at[h % 2, j], xr.at[h % 5, j], xs_sem.at[h % 2, j], xr_sem.at[h, j], x_peer, o
        )

    def product(g, half):
        at = pl.ds(pl.multiple_of(g * tile, tile), tile)
        table_part = leg[half, :, at, :].reshape(slot_dev * tile, LINE * l_dev)
        return at, jnp.dot(spread[g], table_part, preferred_element_type=F32)

    def low_end_copy(h):
        return remote(
            zbs.at[h], zbr.at[h, pl.ds(0, LINE - 1)], zbs_sem.at[h, 0], zbr_sem.at[h, 0],
            mate * PAIR + x, o,
        )

    def low_inner_copy(h, j):
        to_z = (mate, far_end, far_inner)[j]
        return remote(
            zbs.at[h, j], zbr.at[h, (0, 1, 3)[j]], zbs_sem.at[h, j],
            zbr_sem.at[h, (0, 1, 1)[j]], to_z * PAIR + x, o,
        )

    def low_x_copy(h):
        return remote(xbs.at[h], xbr.at[h], xbs_sem.at[h], xbr_sem.at[h], x_peer, o)

    def low_part(h, j, half):
        if half == 0:
            return own_part[h % 3, j, :, pl.ds(m_x, m_dev - m_x), :]
        return far_part[h % 3, j]

    def low_middle(h):
        @pl.when(is_end == 0)
        def _():
            low_end_copy(h).wait_recv()
            for j in (1, 2):
                for half in range(2):
                    value = low_part(h, j, half) + zbr[h, j - 1, half].astype(F32)
                    zbs[h, j, half] = value.astype(BF16)
                low_inner_copy(h, j).start()

    def low_across(h):
        def add(first, second):
            for half in (1, 0):
                value = low_part(h, LINE - 1, half)
                value += zbr[h, first, half].astype(F32) + zbr[h, second, half].astype(F32)
                if half == 0:
                    own_part[h % 3, LINE - 1, :, pl.ds(m_x, m_dev - m_x), :] = value
                else:
                    xbs[h] = value.astype(BF16)
            low_x_copy(h).start()

        @pl.when(is_end == 1)
        def _():
            low_inner_copy(h, 0).wait_recv()
            low_inner_copy(h, 1).wait_recv()
            add(0, 1)

        @pl.when(is_end == 0)
        def _():
            low_inner_copy(h, 2).wait_recv()
            add(2, 3)

    def products(h):
        @pl.when(h == 0)
        def _():
            for j in range(LINE):
                leg_copy(1, j).wait()

        @pl.when(h >= 2)
        def _():
            for j in range(LINE):
                x_copy(h - 2, j).wait_send()

        @pl.loop(0, x_groups)
        def _(g):
            at, value = product(g, 1)
            for j in range(LINE):
                piece = value[:, j * l_dev : (j + 1) * l_dev].reshape(2 * CHUNK, tile, l_dev)
                xs[h % 2, j, :, at, :] = piece.astype(BF16)

        for j in range(LINE):
            x_copy(h, j).start()

        @pl.when(h == 0)
        def _():
            for j in range(LINE):
                leg_copy(0, j).wait()

        @pl.loop(x_groups, groups)
        def _(g):
            low = pl.ds(pl.multiple_of((g - x_groups) * tile, tile), tile)
            for half in range(2):
                at, value = product(g, half)
                for j in range(LINE):
                    piece = value[:, j * l_dev : (j + 1) * l_dev].reshape(2 * CHUNK, tile, l_dev)
                    if half == 0:
                        own_part[h % 3, j, :, at, :] = piece
                    else:
                        far_part[h % 3, j, :, low, :] = piece
                    if j < LINE - 1:
                        zbs[h, j, half, :, low, :] = piece.astype(BF16)

        @pl.when(is_end == 1)
        def _():
            low_end_copy(h).start()

        @pl.when(is_end == 0)
        def _():
            low_inner_copy(h, 0).start()

        @pl.loop(0, x_groups)
        def _(g):
            at, value = product(g, 0)
            for j in range(LINE):
                piece = value[:, j * l_dev : (j + 1) * l_dev].reshape(2 * CHUNK, tile, l_dev)
                own_part[h % 3, j, :, at, :] = piece

    def z_copy(h, j, to_z, slot):
        return remote(
            xr.at[h % 5, j], zr.at[h % 4, slot], zs_sem.at[h, j], zr_sem.at[h, slot],
            to_z * PAIR + x, o,
        )

    def end_copy(h, j):
        return z_copy(h, j, mate, j)

    def inner_copy(h, j):
        return z_copy(h, j, (mate, far_end, far_inner)[j], (0, 1, 3)[j])

    high = pl.ds(0, m_x)

    def first_sums(h):
        for j in range(LINE):
            x_copy(h, j).wait_recv()
            value = own_part[h % 3, j, :, high, :] + xr[h % 5, j].astype(F32)
            if j == LINE - 1:
                own_part[h % 3, j, :, high, :] = value
                continue

            @pl.when(is_end == 1)
            def _():
                xr[h % 5, j] = value.astype(BF16)
                end_copy(h, j).start()

            @pl.when(is_end == 0)
            def _():
                if j == 0:
                    xr[h % 5, j] = value.astype(BF16)
                else:
                    end_copy(h, j - 1).wait_recv()
                    xr[h % 5, j] = (value + zr[h % 4, j - 1].astype(F32)).astype(BF16)
                inner_copy(h, j).start()

    def out_copy(h):
        return pltpu.make_async_copy(stage.at[h % 2], out.at[h], out_sem.at[h % 2])

    def last_sums(h):
        @pl.when(h >= 2)
        def _():
            out_copy(h - 2).wait()

        def add(first, second):
            value = own_part[h % 3, LINE - 1, :, high, :]
            value += zr[h % 4, first].astype(F32) + zr[h % 4, second].astype(F32)
            stage[h % 2, :, high, :] = value

        @pl.when(is_end == 1)
        def _():
            inner_copy(h, 0).wait_recv()
            inner_copy(h, 1).wait_recv()
            add(0, 1)
            for j in range(LINE - 1):
                end_copy(h, j).wait_send()
            low_end_copy(h).wait_send()

        @pl.when(is_end == 0)
        def _():
            end_copy(h, 2).wait_recv()
            inner_copy(h, 2).wait_recv()
            add(2, 3)
            for j in range(LINE - 1):
                inner_copy(h, j).wait_send()
                low_inner_copy(h, j).wait_send()

        low_x_copy(h).wait_recv()
        low = pl.ds(m_x, m_dev - m_x)
        stage[h % 2, :, low, :] = own_part[h % 3, LINE - 1, :, low, :] + xbr[h].astype(F32)
        low_x_copy(h).wait_send()
        out_copy(h).start()

    @pl.loop(0, n + 5)
    def _(t):
        def when(step, delay):
            @pl.when((t >= delay) & (t < n + delay))
            def _():
                step(t - delay)

        when(last_sums, 5)
        when(low_across, 4)
        when(transform, 0)
        when(exchange, 1)
        when(spread_out, 2)
        when(products, 2)
        when(low_middle, 3)
        when(first_sums, 3)

    push_mask.wait_send()

    push_first().wait_send()

    @pl.loop(1, n)
    def _(h):
        push_field(h).wait_send()

    @pl.loop(0, n)
    def _(h):
        for k in range(1, n_blk):
            a_copy(h, k).wait_send()

    for h in (n - 2, n - 1):
        y_copy(h).wait_send()
        out_copy(h).wait()
        for j in range(LINE):
            x_copy(h, j).wait_send()


def fused_body(field, ocean_mask, plan, legendre):
    fields, cyc, lon = field.shape
    slot_dev, m_dev, degrees = legendre.shape
    n_blk = LINE * PAIR
    l_dev = degrees // n_blk
    tile = 16
    groups = m_dev // tile
    n = fields // CHUNK
    rows = CHUNK * cyc
    cap = (cyc + n_blk - 1) // n_blk
    per = CHUNK * cap
    table = jnp.asarray(table_of(lon, m_dev))
    x_groups = groups - max(groups // 8, 1)
    piece = (2 * CHUNK, m_dev, l_dev)
    high = (2 * CHUNK, x_groups * tile, l_dev)
    low = (2 * CHUNK, m_dev - x_groups * tile, l_dev)
    dma = pltpu.SemaphoreType.DMA
    any_spec = pl.BlockSpec(memory_space=pl.ANY)
    vmem_spec = pl.BlockSpec(memory_space=pltpu.VMEM)
    scratch = [
        pltpu.VMEM((2, slot_dev, m_dev, LINE * l_dev), BF16),
        pltpu.VMEM((groups, 2 * CHUNK * tile, slot_dev * tile), BF16),
        pltpu.VMEM((3, LINE) + piece, F32),
        pltpu.VMEM((3, LINE) + low, F32),
        pltpu.VMEM((2, LINE) + high, BF16),
        pltpu.VMEM((5, LINE) + high, BF16),
        pltpu.VMEM((4, 4) + high, BF16),
        pltpu.VMEM((n, LINE - 1, 2) + low, BF16),
        pltpu.VMEM((n, 4, 2) + low, BF16),
        pltpu.VMEM((n,) + low, BF16),
        pltpu.VMEM((n,) + low, BF16),
        pltpu.VMEM((2, lon, 2 * m_dev), BF16),
        pltpu.VMEM((2, lon, 2 * m_dev), BF16),
        pltpu.VMEM((2, CHUNK, cyc, lon), F32),
        pltpu.VMEM((2, CHUNK, cyc, lon), F32),
        pltpu.VMEM((cyc, lon), jnp.int32),
        pltpu.VMEM((cyc, lon), jnp.int32),
        pltpu.VMEM((4 * rows, lon), BF16),
        pltpu.VMEM((2, rows, 2 * m_dev), F32),
        pltpu.VMEM((2, rows, 2 * m_dev), F32),
        pltpu.VMEM((n, rows, 2 * m_dev), F32),
        pltpu.VMEM((n, n_blk, per, 2 * m_dev), BF16),
        pltpu.VMEM((n, n_blk, per, 2 * m_dev), BF16),
        pltpu.VMEM((CHUNK, rows, slot_dev * tile), BF16),
        pltpu.VMEM((rows, rows), BF16),
        pltpu.VMEM((2,) + piece, F32),
        pltpu.VMEM((2, 4, BASE, m_dev), F32),
        dma((2, LINE)),
        dma((2,)),
        dma((2,)),
        dma,
        dma((2,)),
        dma((2,)),
        dma((n,)), dma((n,)),
        dma, dma,
        dma((2,)), dma((n,)),
        dma((n, n_blk - 1)), dma((n, n_blk - 1)),
        dma((2, LINE)), dma((n, LINE)),
        dma((n, 3)), dma((n, 4)),
        dma((n, 3)), dma((n, 2)),
        dma((n,)), dma((n,)),
    ]
    dims = (n, groups, x_groups, tile, m_dev, l_dev, cyc, lon, slot_dev, cap)
    sums, _ = pl.pallas_call(
        functools.partial(fused_kernel, dims),
        out_shape=[
            jax.ShapeDtypeStruct((n,) + piece, F32),
            jax.ShapeDtypeStruct(field.shape, F32),
        ],
        in_specs=[any_spec] * 4 + [vmem_spec],
        out_specs=[any_spec] * 2,
        scratch_shapes=scratch,
        compiler_params=pltpu.CompilerParams(
            collective_id=0, has_side_effects=True, vmem_limit_bytes=66 * 1000 * 1000
        ),
        name="analysis",
    )(field, ocean_mask, legendre, table, plan.reshape(n_blk, cyc))
    sums = sums.reshape(fields, 2, m_dev, l_dev)
    return jnp.transpose(sums, (3, 0, 1, 2))


def fits(mesh, field, legendre):
    shape = dict(mesh.shape)
    n_blk, n_order = shape["blk"], shape["order"]
    cyc, lon = field.shape[1] // n_blk, field.shape[2] // n_order
    slots, m_dev = legendre.shape[0] // n_blk, legendre.shape[1] // n_order
    return (
        n_blk == LINE * PAIR
        and n_order == 4
        and field.shape[0] % CHUNK == 0
        and field.shape[0] // CHUNK >= 5
        and lon == BASE * BASE
        and NLON == 4 * lon
        and m_dev % 128 == 0
        and legendre.shape[2] == n_blk * 128
        and cyc % n_blk == 0
        and slots % 8 == 0
    )


def twiddle(first, count):
    longitudes = first + jnp.arange(count, dtype=jnp.int32)
    orders = jnp.arange(M, dtype=jnp.int32)
    product = longitudes[:, None] * orders[None, :] % NLON
    angle = product.astype(jnp.float32) * (2.0 * math.pi / NLON)
    scale = 1.0 / math.sqrt(NLON)
    return jnp.stack([jnp.cos(angle) * scale, -jnp.sin(angle) * scale], axis=1)


def transform(values, table):
    return jnp.einsum("frn,ncm->frcm", values, table, precision=lax.Precision.HIGHEST)


def pack_cycles(masked, plan, slot_dev):
    n_blk = lax.axis_size("blk")
    own_index = lax.axis_index("blk")
    cycle_dev = masked.shape[1]
    cap = (cycle_dev + n_blk - 1) // n_blk
    grid = plan.reshape(n_blk, cycle_dev)
    owner = grid // slot_dev
    positions = jnp.arange(cycle_dev, dtype=jnp.int32)
    earlier = positions[None, :] < positions[:, None]
    same_owner = owner[:, :, None] == owner[:, None, :]
    rank = jnp.sum(same_owner & earlier[None], axis=2, dtype=jnp.int32)
    send_pos = owner * cap + rank
    local_pos = lax.dynamic_index_in_dim(send_pos, own_index, 0, keepdims=False)
    buffer_ids = jnp.arange(n_blk * cap, dtype=jnp.int32)
    send_onehot = (buffer_ids[:, None] == local_pos[None, :]).astype(jnp.float32)
    outgoing = jnp.einsum("qr,frn->fqn", send_onehot, masked, precision=lax.Precision.HIGHEST)
    arrived = lax.all_to_all(outgoing, "blk", split_axis=1, concat_axis=1, tiled=True)
    source_pos = (jnp.arange(n_blk, dtype=jnp.int32)[:, None] * cap + rank).reshape(-1)
    mine = (owner == own_index).reshape(-1)
    slot_local = (grid % slot_dev).reshape(-1)
    slot_ids = jnp.arange(slot_dev, dtype=jnp.int32)
    slot_onehot = ((slot_local[None, :] == slot_ids[:, None]) & mine[None, :]).astype(jnp.float32)
    source_onehot = (source_pos[:, None] == buffer_ids[None, :]).astype(jnp.float32)
    receive_map = jnp.dot(slot_onehot, source_onehot, precision=lax.Precision.HIGHEST)
    return jnp.einsum("pq,fqn->fpn", receive_map, arrived, precision=lax.Precision.HIGHEST)


def degree_sums(legendre, spectrum):
    n_blk = lax.axis_size("blk")
    own_index = lax.axis_index("blk")
    pairs = n_blk // 2
    degree_dev = legendre.shape[2] // n_blk
    own_pair, own_side = own_index // 2, own_index % 2
    swap = [(i, i + 1 - 2 * (i % 2)) for i in range(n_blk)]

    def terms_for(target):
        table = lax.dynamic_slice_in_dim(legendre, target * degree_dev, degree_dev, 2)
        return jnp.einsum("pml,fpcm->lfcm", table, spectrum, preferred_element_type=jnp.float32)

    def pair_sum(step):
        base = (own_pair + step) % pairs * 2
        given = terms_for(base + 1 - own_side).astype(jnp.bfloat16)
        taken = lax.ppermute(given, "blk", swap)
        return terms_for(base + own_side) + taken.astype(jnp.float32)

    steps = sorted(range(1, pairs), key=lambda step: abs(2 * step - pairs))
    arrived = []
    for step in steps:
        shift = [(i, (i + 2 * step) % n_blk) for i in range(n_blk)]
        arrived.append(lax.ppermute(pair_sum(step).astype(jnp.bfloat16), "blk", shift))
    total = pair_sum(0)
    for piece in arrived:
        total = total + piece.astype(jnp.float32)
    return total


def body(field, ocean_mask, plan, legendre):
    lon_local = field.shape[2]
    slot_dev = legendre.shape[0]
    masked = field * ocean_mask.astype(jnp.float32)[None]
    packed = pack_cycles(masked, plan, slot_dev)
    first = lax.axis_index("order") * lon_local
    terms = transform(packed, twiddle(first, lon_local))
    spectrum = lax.psum_scatter(terms, "order", scatter_dimension=3, tiled=True).astype(
        jnp.bfloat16
    )
    coefficients = degree_sums(legendre, spectrum)
    return coefficients


def solution(mesh):
    placed = (P(None, "blk", "order"), P("blk", "order"), P(), P("blk", "order", None))

    def run(field, ocean_mask, plan, legendre):
        chosen = fused_body if fits(mesh, field, legendre) else body
        mapped = jax.shard_map(
            chosen, mesh=mesh, in_specs=placed, out_specs=P("blk", None, None, "order"),
            check_vma=False,
        )
        return mapped(field, ocean_mask, plan, legendre)

    return run
```

```python
import functools
import math

import jax
import jax.numpy as jnp
import numpy as np
from jax import lax
from jax.experimental import pallas as pl
from jax.experimental.pallas import tpu as pltpu
from jax.sharding import PartitionSpec as P

NLON = 4096
M = 1024
MESH = pl.DeviceIdType.MESH
F32, BF16 = jnp.float32, jnp.bfloat16

LINE, PAIR = 4, 2
CHUNK = 2
BASE = 32


def table_of(lon_local, orders):
    coarse = np.arange(lon_local // BASE)[:, None] * BASE
    fine = np.arange(BASE)[:, None]
    m = np.arange(M)[None, :]

    def parts(n, scale):
        angle = (n * m % NLON) * (2.0 * math.pi / NLON)
        return [np.cos(angle) * scale, np.sin(angle) * scale]

    both = parts(coarse, 1.0) + parts(fine, 1.0 / math.sqrt(NLON))
    owners = M // orders
    stacked = np.stack([t.reshape(BASE, owners, orders) for t in both])
    return stacked.transpose(2, 0, 1, 3).astype(np.float32)


def fused_kernel(
    dims,
    field, mask, legendre, table, plan,
    out, far_field,
    leg, spread, own_part, far_part, xs, xr, zr, zbs, zbr, xbs, xbr, wh, wl, near, far, mask_near, mask_far, parts,
    y_own, y_send, y_recv, a_send, a_recv, pick, pack, stage, tabs,
    leg_sem, near_sem, far_sem, mask_sem, tab_sem, out_sem,
    pf_send, pf_recv, pm_send, pm_recv, ys_sem, yr_sem, as_sem, ar_sem,
    xs_sem, xr_sem, zs_sem, zr_sem, zbs_sem, zbr_sem, xbs_sem, xbr_sem,
):
    n, groups, x_groups, tile, m_dev, l_dev, cyc, lon, slot_dev, cap = dims
    m_x = x_groups * tile
    rows = CHUNK * cyc
    n_blk = LINE * PAIR
    b = lax.axis_index("blk")
    o = lax.axis_index("order")
    z, x = b // PAIR, b % PAIR
    side = z // 2
    odd = z % 2
    is_end = 1 - (odd + side - 2 * odd * side)
    far_end = (LINE - 1) * (1 - side)
    far_inner = 2 - side
    mate = 2 * side + 1 - odd
    dest = [
        is_end * far_end + (1 - is_end) * mate,
        is_end * far_inner + (1 - is_end) * far_end,
        is_end * mate + (1 - is_end) * far_inner,
        z,
    ]
    x_peer = b + 1 - 2 * x
    y_peer = (o + 2) % 4
    c_peer = o + 1 - 2 * (o % 2)

    def remote(src, dst, send, recv, blk, order):
        return pltpu.make_async_remote_copy(
            src_ref=src, dst_ref=dst, send_sem=send, recv_sem=recv,
            device_id=(blk, order), device_id_type=MESH,
        )

    def leg_copy(half, j):
        block = dest[j] * PAIR + (x if half == 0 else 1 - x)
        lanes = pl.ds(pl.multiple_of(block * l_dev, l_dev), l_dev)
        return pltpu.make_async_copy(
            legendre.at[:, :, lanes],
            leg.at[half, :, :, pl.ds(j * l_dev, l_dev)],
            leg_sem.at[half, j],
        )

    def near_copy(h):
        return pltpu.make_async_copy(
            field.at[pl.ds(h * CHUNK, CHUNK)], near.at[h % 2], near_sem.at[h % 2]
        )

    def far_copy(h):
        return pltpu.make_async_copy(
            far_field.at[pl.ds(h * CHUNK, CHUNK)], far.at[h % 2], far_sem.at[h % 2]
        )

    def push_field(h):
        fields = pl.ds(h * CHUNK, CHUNK)
        return remote(
            field.at[fields], far_field.at[fields], pf_send.at[h], pf_recv.at[h], b, c_peer
        )

    def push_first(h):
        return remote(
            field.at[pl.ds(h * CHUNK, CHUNK)], far.at[h], pf_send.at[h], pf_recv.at[h], b, c_peer
        )

    tab_own = pltpu.make_async_copy(table.at[o], tabs.at[0], tab_sem.at[0])
    tab_other = pltpu.make_async_copy(table.at[y_peer], tabs.at[1], tab_sem.at[1])
    tab_own.start()
    tab_other.start()
    mask_own = pltpu.make_async_copy(mask, mask_near, mask_sem)
    mask_own.start()
    near_copy(0).start()
    near_copy(1).start()

    barrier = pltpu.get_barrier_semaphore()
    for k in range(1, n_blk):
        pl.semaphore_signal(barrier, inc=1, device_id=((b + k) % n_blk, o), device_id_type=MESH)
    pl.semaphore_signal(barrier, inc=1, device_id=(b, y_peer), device_id_type=MESH)
    pl.semaphore_signal(barrier, inc=1, device_id=(b, c_peer), device_id_type=MESH)

    def iota(shape, axis):
        return lax.broadcasted_iota(jnp.int32, shape, axis)

    wanted = (b * slot_dev + iota((1, slot_dev * tile), 1) // tile).astype(F32)
    row_id, col_id = iota((cyc, cyc), 0), iota((cyc, cyc), 1)
    send_at = jnp.zeros((1, cyc), F32)
    source = jnp.zeros((cyc, slot_dev * tile), F32)
    for block in range(n_blk):
        across = plan[pl.ds(block, 1), :].astype(F32)
        down = jnp.sum(jnp.where(row_id == col_id, across, 0.0), axis=1, keepdims=True)
        owner_across = jnp.floor((across + 0.5) * (1.0 / slot_dev))
        owner_down = jnp.floor((down + 0.5) * (1.0 / slot_dev))
        same = owner_down == owner_across
        rank_across = jnp.sum(
            jnp.where(same & (row_id < col_id), 1.0, 0.0), axis=0, keepdims=True
        )
        rank_down = jnp.sum(
            jnp.where(same & (col_id < row_id), 1.0, 0.0), axis=1, keepdims=True
        )
        here = jnp.where(b == block, 1.0, 0.0)
        send_at += here * (owner_across * cap + rank_across)
        source += jnp.where(down == wanted, block * cap + rank_down, 0.0)
    source = jnp.sum(source, axis=0, keepdims=True)
    per = CHUNK * cap
    r = iota((rows, cyc), 0)
    position = (r // per * cap + r % cap).astype(F32)
    for f in range(CHUNK):
        hit = (position == send_at) & (r % per // cap == f)
        pack[:, pl.ds(f * cyc, cyc)] = jnp.where(hit, 1.0, 0.0).astype(BF16)
    r = iota((rows, slot_dev * tile), 0)
    position = (r // per * cap + r % cap).astype(F32)
    for f in range(CHUNK):
        hit = (position == source) & (r % per // cap == f)
        pick[f] = jnp.where(hit, 1.0, 0.0).astype(BF16)

    pl.semaphore_wait(barrier, n_blk + 1)

    push_mask = remote(mask, mask_far, pm_send, pm_recv, b, c_peer)
    push_mask.start()
    push_first(0).start()
    push_first(1).start()

    @pl.loop(2, n)
    def _(h):
        push_field(h).start()

    tab_own.wait()
    tab_other.wait()
    for side_of in range(2):

        @pl.loop(0, lon // BASE)
        def _(a):
            ca = tabs[side_of, 0, pl.ds(a, 1), :]
            sa = tabs[side_of, 1, pl.ds(a, 1), :]
            cb = tabs[side_of, 2]
            sb = tabs[side_of, 3]
            at = pl.ds(pl.multiple_of(a * BASE, BASE), BASE)
            for c, value in enumerate((ca * cb - sa * sb, -(sa * cb + ca * sb))):
                high = value.astype(BF16)
                wh[side_of, at, pl.ds(c * m_dev, m_dev)] = high
                rest = value - high.astype(F32)
                wl[side_of, at, pl.ds(c * m_dev, m_dev)] = rest.astype(BF16)

    mask_own.wait()
    push_mask.wait()

    def turn(index):
        quarter = (index * iota((1, m_dev), 1)) % 4
        real = jnp.where(quarter == 0, 1.0, jnp.where(quarter == 2, -1.0, 0.0))
        imag = jnp.where(quarter == 3, 1.0, jnp.where(quarter == 1, -1.0, 0.0))
        return real, imag

    def y_copy(h):
        return remote(y_send.at[h % 2], y_recv.at[h], ys_sem.at[h % 2], yr_sem.at[h], b, y_peer)

    def transform(h):
        near_copy(h).wait()

        @pl.when(h < 2)
        def _():
            push_first(h).wait()

        @pl.when(h == 0)
        def _():
            for half in (1, 0):
                for j in range(LINE):
                    leg_copy(half, j).start()

        @pl.when(h >= 2)
        def _():
            far_copy(h).wait()

        @pl.when((h >= 1) & (h + 1 < n))
        def _():
            near_copy(h + 1).start()
            push_field(h + 1).wait()
            far_copy(h + 1).start()

        @pl.when(h >= 2)
        def _():
            y_copy(h - 2).wait_send()

        for i, (data, wet) in enumerate(((near, mask_near), (far, mask_far))):
            value = (data[h % 2] * wet[...].astype(F32)[None]).reshape(rows, lon)
            high = value.astype(BF16)
            parts[pl.ds(i * rows, rows), :] = high
            rest = value - high.astype(F32)
            parts[pl.ds((2 + i) * rows, rows), :] = rest.astype(BF16)
        near_r, near_i = turn(o)
        far_r, far_i = turn(c_peer)
        for side_of in (1, 0):
            both = jnp.dot(parts[...], wh[side_of], preferred_element_type=F32)
            total = both[: 2 * rows] + both[2 * rows :]
            total += jnp.dot(
                parts[pl.ds(0, 2 * rows), :], wl[side_of], preferred_element_type=F32
            )
            nr, ni = total[:rows, :m_dev], total[:rows, m_dev:]
            fr, fi = total[rows:, :m_dev], total[rows:, m_dev:]
            real = near_r * nr - near_i * ni + far_r * fr - far_i * fi
            imag = near_r * ni + near_i * nr + far_r * fi + far_i * fr
            target = y_send if side_of else y_own
            target[h % 2, :, pl.ds(0, m_dev)] = real
            target[h % 2, :, pl.ds(m_dev, m_dev)] = imag
            if side_of:
                y_copy(h).start()

    def a_copy(h, k):
        to = (b + k) % n_blk
        return remote(
            a_send.at[h, to], a_recv.at[h, b], as_sem.at[h, k - 1], ar_sem.at[h, k - 1], to, o
        )

    def exchange(h):
        y_copy(h).wait_recv()
        spectrum = (y_own[h % 2] + y_recv[h]).astype(BF16)
        packed = jnp.dot(pack[...], spectrum, preferred_element_type=F32).astype(BF16)
        a_send[h] = packed.reshape(n_blk, per, 2 * m_dev)
        a_recv[h, b] = a_send[h, b]
        for k in range(1, n_blk):
            a_copy(h, k).start()

    diagonal = (iota((1, tile, slot_dev * tile), 1)) == (iota((1, tile, slot_dev * tile), 2) % tile)

    def spread_out(h):
        for k in range(1, n_blk):
            a_copy(h, k).wait()
        got = a_recv[h].reshape(rows, 2 * m_dev)
        for c in range(2):
            for f in range(CHUNK):
                value = lax.dot_general(
                    got[:, c * m_dev : (c + 1) * m_dev], pick[f],
                    (((0,), (0,)), ((), ())), preferred_element_type=F32,
                )
                value = value.reshape(groups, tile, slot_dev * tile)
                spread[:, pl.ds((f * 2 + c) * tile, tile), :] = jnp.where(
                    diagonal, value, 0.0
                ).astype(BF16)

    def x_copy(h, j):
        return remote(
            xs.at[h % 2, j], xr.at[h % 5, j], xs_sem.at[h % 2, j], xr_sem.at[h, j], x_peer, o
        )

    def product(g, half, first=0, count=LINE):
        at = pl.ds(pl.multiple_of(g * tile, tile), tile)
        lanes = pl.ds(first * l_dev, count * l_dev)
        table_part = leg[half, :, at, lanes].reshape(slot_dev * tile, count * l_dev)
        return at, jnp.dot(spread[g], table_part, preferred_element_type=F32)

    def low_end_copy(h):
        return remote(
            zbs.at[h], zbr.at[h, pl.ds(0, LINE - 1)], zbs_sem.at[h, 0], zbr_sem.at[h, 0],
            mate * PAIR + x, o,
        )

    def low_inner_copy(h, j):
        to_z = (mate, far_end, far_inner)[j]
        return remote(
            zbs.at[h, j], zbr.at[h, (0, 1, 3)[j]], zbs_sem.at[h, j],
            zbr_sem.at[h, (0, 1, 1)[j]], to_z * PAIR + x, o,
        )

    def low_x_copy(h):
        return remote(xbs.at[h], xbr.at[h], xbs_sem.at[h], xbr_sem.at[h], x_peer, o)

    def low_part(h, j, half):
        if half == 0:
            return own_part[h % 3, j, :, pl.ds(m_x, m_dev - m_x), :]
        return far_part[h % 3, j]

    def low_middle(h):
        @pl.when(is_end == 0)
        def _():
            low_end_copy(h).wait_recv()
            for j in (1, 2):
                for half in range(2):
                    value = low_part(h, j, half) + zbr[h, j - 1, half].astype(F32)
                    zbs[h, j, half] = value.astype(BF16)
                low_inner_copy(h, j).start()

    def low_across(h):
        def add(first, second):
            for half in (1, 0):
                value = low_part(h, LINE - 1, half)
                value += zbr[h, first, half].astype(F32) + zbr[h, second, half].astype(F32)
                if half == 0:
                    own_part[h % 3, LINE - 1, :, pl.ds(m_x, m_dev - m_x), :] = value
                else:
                    xbs[h] = value.astype(BF16)
            low_x_copy(h).start()

        @pl.when(is_end == 1)
        def _():
            low_inner_copy(h, 0).wait_recv()
            low_inner_copy(h, 1).wait_recv()
            add(0, 1)

        @pl.when(is_end == 0)
        def _():
            low_inner_copy(h, 2).wait_recv()
            add(2, 3)

    def products(h):
        @pl.when(h == 0)
        def _():
            for j in range(LINE):
                leg_copy(1, j).wait()

        @pl.when(h >= 2)
        def _():
            for j in range(LINE):
                x_copy(h - 2, j).wait_send()

        def x_products(first, count):
            @pl.loop(0, x_groups)
            def _(g):
                at, value = product(g, 1, first, count)
                for j in range(count):
                    piece = value[:, j * l_dev : (j + 1) * l_dev].reshape(2 * CHUNK, tile, l_dev)
                    xs[h % 2, first + j, :, at, :] = piece.astype(BF16)

            for j in range(count):
                x_copy(h, first + j).start()

        @pl.when(h == 0)
        def _():
            x_products(0, 2)
            x_products(2, 2)

        @pl.when(h > 0)
        def _():
            x_products(0, LINE)

        @pl.when(h == 0)
        def _():
            for j in range(LINE):
                leg_copy(0, j).wait()

        @pl.loop(x_groups, groups)
        def _(g):
            low = pl.ds(pl.multiple_of((g - x_groups) * tile, tile), tile)
            for half in range(2):
                at, value = product(g, half)
                for j in range(LINE):
                    piece = value[:, j * l_dev : (j + 1) * l_dev].reshape(2 * CHUNK, tile, l_dev)
                    if half == 0:
                        own_part[h % 3, j, :, at, :] = piece
                    else:
                        far_part[h % 3, j, :, low, :] = piece
                    if j < LINE - 1:
                        zbs[h, j, half, :, low, :] = piece.astype(BF16)

        @pl.when(is_end == 1)
        def _():
            low_end_copy(h).start()

        @pl.when(is_end == 0)
        def _():
            low_inner_copy(h, 0).start()

        @pl.loop(0, x_groups)
        def _(g):
            at, value = product(g, 0)
            for j in range(LINE):
                piece = value[:, j * l_dev : (j + 1) * l_dev].reshape(2 * CHUNK, tile, l_dev)
                own_part[h % 3, j, :, at, :] = piece

    def z_copy(h, j, to_z, slot):
        return remote(
            xr.at[h % 5, j], zr.at[h % 4, slot], zs_sem.at[h, j], zr_sem.at[h, slot],
            to_z * PAIR + x, o,
        )

    def end_copy(h, j):
        return z_copy(h, j, mate, j)

    def inner_copy(h, j):
        return z_copy(h, j, (mate, far_end, far_inner)[j], (0, 1, 3)[j])

    high = pl.ds(0, m_x)

    def first_sums(h):
        for j in range(LINE):
            if j == LINE - 1:

                @pl.when(h == n - 1)
                def _():
                    low_across(h)

            x_copy(h, j).wait_recv()
            value = own_part[h % 3, j, :, high, :] + xr[h % 5, j].astype(F32)
            if j == LINE - 1:
                own_part[h % 3, j, :, high, :] = value
                continue

            @pl.when(is_end == 1)
            def _():
                xr[h % 5, j] = value.astype(BF16)
                end_copy(h, j).start()

            @pl.when(is_end == 0)
            def _():
                if j == 0:
                    xr[h % 5, j] = value.astype(BF16)
                else:
                    end_copy(h, j - 1).wait_recv()
                    xr[h % 5, j] = (value + zr[h % 4, j - 1].astype(F32)).astype(BF16)
                inner_copy(h, j).start()

    def out_copy(h):
        return pltpu.make_async_copy(stage.at[h % 2], out.at[h], out_sem.at[h % 2])

    def last_sums(h):
        @pl.when(h >= 2)
        def _():
            out_copy(h - 2).wait()

        def add(first, second):
            value = own_part[h % 3, LINE - 1, :, high, :]
            value += zr[h % 4, first].astype(F32) + zr[h % 4, second].astype(F32)
            stage[h % 2, :, high, :] = value

        @pl.when(is_end == 1)
        def _():
            inner_copy(h, 0).wait_recv()
            inner_copy(h, 1).wait_recv()
            add(0, 1)
            for j in range(LINE - 1):
                end_copy(h, j).wait_send()
            low_end_copy(h).wait_send()

        @pl.when(is_end == 0)
        def _():
            end_copy(h, 2).wait_recv()
            inner_copy(h, 2).wait_recv()
            add(2, 3)
            for j in range(LINE - 1):
                inner_copy(h, j).wait_send()
                low_inner_copy(h, j).wait_send()

        low_x_copy(h).wait_recv()
        low = pl.ds(m_x, m_dev - m_x)
        stage[h % 2, :, low, :] = own_part[h % 3, LINE - 1, :, low, :] + xbr[h].astype(F32)
        low_x_copy(h).wait_send()
        out_copy(h).start()

    @pl.loop(0, n + 5)
    def _(t):
        def when(step, delay):
            @pl.when((t >= delay) & (t < n + delay))
            def _():
                step(t - delay)

        when(last_sums, 5)

        @pl.when((t >= 4) & (t < n + 3))
        def _():
            low_across(t - 4)

        when(transform, 0)
        when(exchange, 1)
        when(spread_out, 2)
        when(products, 2)
        when(low_middle, 3)
        when(first_sums, 3)

    for h in (n - 2, n - 1):
        y_copy(h).wait_send()
        out_copy(h).wait()
        for j in range(LINE):
            x_copy(h, j).wait_send()


def fused_body(field, ocean_mask, plan, legendre):
    fields, cyc, lon = field.shape
    slot_dev, m_dev, degrees = legendre.shape
    n_blk = LINE * PAIR
    l_dev = degrees // n_blk
    tile = 16
    groups = m_dev // tile
    n = fields // CHUNK
    rows = CHUNK * cyc
    cap = (cyc + n_blk - 1) // n_blk
    per = CHUNK * cap
    table = jnp.asarray(table_of(lon, m_dev))
    x_groups = groups - max(groups // 8, 1)
    piece = (2 * CHUNK, m_dev, l_dev)
    high = (2 * CHUNK, x_groups * tile, l_dev)
    low = (2 * CHUNK, m_dev - x_groups * tile, l_dev)
    dma = pltpu.SemaphoreType.DMA
    any_spec = pl.BlockSpec(memory_space=pl.ANY)
    vmem_spec = pl.BlockSpec(memory_space=pltpu.VMEM)
    scratch = [
        pltpu.VMEM((2, slot_dev, m_dev, LINE * l_dev), BF16),
        pltpu.VMEM((groups, 2 * CHUNK * tile, slot_dev * tile), BF16),
        pltpu.VMEM((3, LINE) + piece, F32),
        pltpu.VMEM((3, LINE) + low, F32),
        pltpu.VMEM((2, LINE) + high, BF16),
        pltpu.VMEM((5, LINE) + high, BF16),
        pltpu.VMEM((4, 4) + high, BF16),
        pltpu.VMEM((n, LINE - 1, 2) + low, BF16),
        pltpu.VMEM((n, 4, 2) + low, BF16),
        pltpu.VMEM((n,) + low, BF16),
        pltpu.VMEM((n,) + low, BF16),
        pltpu.VMEM((2, lon, 2 * m_dev), BF16),
        pltpu.VMEM((2, lon, 2 * m_dev), BF16),
        pltpu.VMEM((2, CHUNK, cyc, lon), F32),
        pltpu.VMEM((2, CHUNK, cyc, lon), F32),
        pltpu.VMEM((cyc, lon), jnp.int32),
        pltpu.VMEM((cyc, lon), jnp.int32),
        pltpu.VMEM((4 * rows, lon), BF16),
        pltpu.VMEM((2, rows, 2 * m_dev), F32),
        pltpu.VMEM((2, rows, 2 * m_dev), F32),
        pltpu.VMEM((n, rows, 2 * m_dev), F32),
        pltpu.VMEM((n, n_blk, per, 2 * m_dev), BF16),
        pltpu.VMEM((n, n_blk, per, 2 * m_dev), BF16),
        pltpu.VMEM((CHUNK, rows, slot_dev * tile), BF16),
        pltpu.VMEM((rows, rows), BF16),
        pltpu.VMEM((2,) + piece, F32),
        pltpu.VMEM((2, 4, BASE, m_dev), F32),
        dma((2, LINE)),
        dma((2,)),
        dma((2,)),
        dma,
        dma((2,)),
        dma((2,)),
        dma((n,)), dma((n,)),
        dma, dma,
        dma((2,)), dma((n,)),
        dma((n, n_blk - 1)), dma((n, n_blk - 1)),
        dma((2, LINE)), dma((n, LINE)),
        dma((n, 3)), dma((n, 4)),
        dma((n, 3)), dma((n, 2)),
        dma((n,)), dma((n,)),
    ]
    dims = (n, groups, x_groups, tile, m_dev, l_dev, cyc, lon, slot_dev, cap)
    sums, _ = pl.pallas_call(
        functools.partial(fused_kernel, dims),
        out_shape=[
            jax.ShapeDtypeStruct((n,) + piece, F32),
            jax.ShapeDtypeStruct(field.shape, F32),
        ],
        in_specs=[any_spec] * 4 + [vmem_spec],
        out_specs=[any_spec] * 2,
        scratch_shapes=scratch,
        compiler_params=pltpu.CompilerParams(
            collective_id=0, has_side_effects=True, vmem_limit_bytes=66 * 1000 * 1000
        ),
        name="analysis",
    )(field, ocean_mask, legendre, table, plan.reshape(n_blk, cyc))
    sums = sums.reshape(fields, 2, m_dev, l_dev)
    return jnp.transpose(sums, (3, 0, 1, 2))


def fits(mesh, field, legendre):
    shape = dict(mesh.shape)
    n_blk, n_order = shape["blk"], shape["order"]
    cyc, lon = field.shape[1] // n_blk, field.shape[2] // n_order
    slots, m_dev = legendre.shape[0] // n_blk, legendre.shape[1] // n_order
    return (
        n_blk == LINE * PAIR
        and n_order == 4
        and field.shape[0] % CHUNK == 0
        and field.shape[0] // CHUNK >= 5
        and lon == BASE * BASE
        and NLON == 4 * lon
        and m_dev % 128 == 0
        and legendre.shape[2] == n_blk * 128
        and cyc % n_blk == 0
        and slots % 8 == 0
    )


def twiddle(first, count):
    longitudes = first + jnp.arange(count, dtype=jnp.int32)
    orders = jnp.arange(M, dtype=jnp.int32)
    product = longitudes[:, None] * orders[None, :] % NLON
    angle = product.astype(jnp.float32) * (2.0 * math.pi / NLON)
    scale = 1.0 / math.sqrt(NLON)
    return jnp.stack([jnp.cos(angle) * scale, -jnp.sin(angle) * scale], axis=1)


def transform(values, table):
    return jnp.einsum("frn,ncm->frcm", values, table, precision=lax.Precision.HIGHEST)


def pack_cycles(masked, plan, slot_dev):
    n_blk = lax.axis_size("blk")
    own_index = lax.axis_index("blk")
    cycle_dev = masked.shape[1]
    cap = (cycle_dev + n_blk - 1) // n_blk
    grid = plan.reshape(n_blk, cycle_dev)
    owner = grid // slot_dev
    positions = jnp.arange(cycle_dev, dtype=jnp.int32)
    earlier = positions[None, :] < positions[:, None]
    same_owner = owner[:, :, None] == owner[:, None, :]
    rank = jnp.sum(same_owner & earlier[None], axis=2, dtype=jnp.int32)
    send_pos = owner * cap + rank
    local_pos = lax.dynamic_index_in_dim(send_pos, own_index, 0, keepdims=False)
    buffer_ids = jnp.arange(n_blk * cap, dtype=jnp.int32)
    send_onehot = (buffer_ids[:, None] == local_pos[None, :]).astype(jnp.float32)
    outgoing = jnp.einsum("qr,frn->fqn", send_onehot, masked, precision=lax.Precision.HIGHEST)
    arrived = lax.all_to_all(outgoing, "blk", split_axis=1, concat_axis=1, tiled=True)
    source_pos = (jnp.arange(n_blk, dtype=jnp.int32)[:, None] * cap + rank).reshape(-1)
    mine = (owner == own_index).reshape(-1)
    slot_local = (grid % slot_dev).reshape(-1)
    slot_ids = jnp.arange(slot_dev, dtype=jnp.int32)
    slot_onehot = ((slot_local[None, :] == slot_ids[:, None]) & mine[None, :]).astype(jnp.float32)
    source_onehot = (source_pos[:, None] == buffer_ids[None, :]).astype(jnp.float32)
    receive_map = jnp.dot(slot_onehot, source_onehot, precision=lax.Precision.HIGHEST)
    return jnp.einsum("pq,fqn->fpn", receive_map, arrived, precision=lax.Precision.HIGHEST)


def degree_sums(legendre, spectrum):
    n_blk = lax.axis_size("blk")
    own_index = lax.axis_index("blk")
    pairs = n_blk // 2
    degree_dev = legendre.shape[2] // n_blk
    own_pair, own_side = own_index // 2, own_index % 2
    swap = [(i, i + 1 - 2 * (i % 2)) for i in range(n_blk)]

    def terms_for(target):
        table = lax.dynamic_slice_in_dim(legendre, target * degree_dev, degree_dev, 2)
        return jnp.einsum("pml,fpcm->lfcm", table, spectrum, preferred_element_type=jnp.float32)

    def pair_sum(step):
        base = (own_pair + step) % pairs * 2
        given = terms_for(base + 1 - own_side).astype(jnp.bfloat16)
        taken = lax.ppermute(given, "blk", swap)
        return terms_for(base + own_side) + taken.astype(jnp.float32)

    steps = sorted(range(1, pairs), key=lambda step: abs(2 * step - pairs))
    arrived = []
    for step in steps:
        shift = [(i, (i + 2 * step) % n_blk) for i in range(n_blk)]
        arrived.append(lax.ppermute(pair_sum(step).astype(jnp.bfloat16), "blk", shift))
    total = pair_sum(0)
    for piece in arrived:
        total = total + piece.astype(jnp.float32)
    return total


def body(field, ocean_mask, plan, legendre):
    lon_local = field.shape[2]
    slot_dev = legendre.shape[0]
    masked = field * ocean_mask.astype(jnp.float32)[None]
    packed = pack_cycles(masked, plan, slot_dev)
    first = lax.axis_index("order") * lon_local
    terms = transform(packed, twiddle(first, lon_local))
    spectrum = lax.psum_scatter(terms, "order", scatter_dimension=3, tiled=True).astype(
        jnp.bfloat16
    )
    coefficients = degree_sums(legendre, spectrum)
    return coefficients


def solution(mesh):
    placed = (P(None, "blk", "order"), P("blk", "order"), P(), P("blk", "order", None))

    def run(field, ocean_mask, plan, legendre):
        chosen = fused_body if fits(mesh, field, legendre) else body
        mapped = jax.shard_map(
            chosen, mesh=mesh, in_specs=placed, out_specs=P("blk", None, None, "order"),
            check_vma=False,
        )
        return mapped(field, ocean_mask, plan, legendre)

    return run
```

```python
import functools
import math

import jax
import jax.numpy as jnp
import numpy as np
from jax import lax
from jax.experimental import pallas as pl
from jax.experimental.pallas import tpu as pltpu
from jax.sharding import PartitionSpec as P

NLON = 4096
M = 1024
MESH = pl.DeviceIdType.MESH
F32, BF16 = jnp.float32, jnp.bfloat16

LINE, PAIR = 4, 2
CHUNK = 2
BASE = 32


def table_of(lon_local, orders):
    coarse = np.arange(lon_local // BASE)[:, None] * BASE
    fine = np.arange(BASE)[:, None]
    m = np.arange(M)[None, :]

    def parts(n, scale):
        angle = (n * m % NLON) * (2.0 * math.pi / NLON)
        return [np.cos(angle) * scale, np.sin(angle) * scale]

    both = parts(coarse, 1.0) + parts(fine, 1.0 / math.sqrt(NLON))
    owners = M // orders
    stacked = np.stack([t.reshape(BASE, owners, orders) for t in both])
    return stacked.transpose(2, 0, 1, 3).astype(np.float32)


def fused_kernel(
    dims,
    field, mask, legendre, table, plan,
    out, far_field,
    leg, spread, own_part, far_part, xs, xr, zr, zbs, zbr, xbs, xbr, wh, wl, near, far, mask_near, mask_far, parts,
    y_own, y_send, y_recv, a_send, a_recv, pick, pack, stage, tabs,
    leg_sem, near_sem, far_sem, mask_sem, tab_sem, out_sem,
    pf_send, pf_recv, pm_send, pm_recv, ys_sem, yr_sem, as_sem, ar_sem,
    xs_sem, xr_sem, zs_sem, zr_sem, zbs_sem, zbr_sem, xbs_sem, xbr_sem,
):
    n, groups, x_groups, tile, m_dev, l_dev, cyc, lon, slot_dev, cap = dims
    m_x = x_groups * tile
    rows = CHUNK * cyc
    n_blk = LINE * PAIR
    b = lax.axis_index("blk")
    o = lax.axis_index("order")
    z, x = b // PAIR, b % PAIR
    side = z // 2
    odd = z % 2
    is_end = 1 - (odd + side - 2 * odd * side)
    far_end = (LINE - 1) * (1 - side)
    far_inner = 2 - side
    mate = 2 * side + 1 - odd
    dest = [
        is_end * far_end + (1 - is_end) * mate,
        is_end * far_inner + (1 - is_end) * far_end,
        is_end * mate + (1 - is_end) * far_inner,
        z,
    ]
    x_peer = b + 1 - 2 * x
    y_peer = (o + 2) % 4
    c_peer = o + 1 - 2 * (o % 2)

    def remote(src, dst, send, recv, blk, order):
        return pltpu.make_async_remote_copy(
            src_ref=src, dst_ref=dst, send_sem=send, recv_sem=recv,
            device_id=(blk, order), device_id_type=MESH,
        )

    def leg_copy(half, j):
        block = dest[j] * PAIR + (x if half == 0 else 1 - x)
        lanes = pl.ds(pl.multiple_of(block * l_dev, l_dev), l_dev)
        return pltpu.make_async_copy(
            legendre.at[:, :, lanes],
            leg.at[half, :, :, pl.ds(j * l_dev, l_dev)],
            leg_sem.at[half, j],
        )

    def near_copy(h):
        return pltpu.make_async_copy(
            field.at[pl.ds(h * CHUNK, CHUNK)], near.at[h % 2], near_sem.at[h % 2]
        )

    def far_copy(h):
        return pltpu.make_async_copy(
            far_field.at[pl.ds(h * CHUNK, CHUNK)], far.at[h % 2], far_sem.at[h % 2]
        )

    def push_field(h):
        fields = pl.ds(h * CHUNK, CHUNK)
        return remote(
            field.at[fields], far_field.at[fields], pf_send.at[h], pf_recv.at[h], b, c_peer
        )

    def push_first(h):
        return remote(
            field.at[pl.ds(h * CHUNK, CHUNK)], far.at[h], pf_send.at[h], pf_recv.at[h], b, c_peer
        )

    tab_own = pltpu.make_async_copy(table.at[o], tabs.at[0], tab_sem.at[0])
    tab_other = pltpu.make_async_copy(table.at[y_peer], tabs.at[1], tab_sem.at[1])
    tab_own.start()
    tab_other.start()
    mask_own = pltpu.make_async_copy(mask, mask_near, mask_sem)
    mask_own.start()
    near_copy(0).start()
    near_copy(1).start()

    barrier = pltpu.get_barrier_semaphore()
    for k in range(1, n_blk):
        pl.semaphore_signal(barrier, inc=1, device_id=((b + k) % n_blk, o), device_id_type=MESH)
    pl.semaphore_signal(barrier, inc=1, device_id=(b, y_peer), device_id_type=MESH)
    pl.semaphore_signal(barrier, inc=1, device_id=(b, c_peer), device_id_type=MESH)

    def iota(shape, axis):
        return lax.broadcasted_iota(jnp.int32, shape, axis)

    wanted = (b * slot_dev + iota((1, slot_dev * tile), 1) // tile).astype(F32)
    row_id, col_id = iota((cyc, cyc), 0), iota((cyc, cyc), 1)
    send_at = jnp.zeros((1, cyc), F32)
    source = jnp.zeros((cyc, slot_dev * tile), F32)
    for block in range(n_blk):
        across = plan[:, pl.ds(block * cyc, cyc)].astype(F32)
        down = jnp.sum(jnp.where(row_id == col_id, across, 0.0), axis=1, keepdims=True)
        owner_across = jnp.floor((across + 0.5) * (1.0 / slot_dev))
        owner_down = jnp.floor((down + 0.5) * (1.0 / slot_dev))
        same = owner_down == owner_across
        rank_across = jnp.sum(
            jnp.where(same & (row_id < col_id), 1.0, 0.0), axis=0, keepdims=True
        )
        rank_down = jnp.sum(
            jnp.where(same & (col_id < row_id), 1.0, 0.0), axis=1, keepdims=True
        )
        here = jnp.where(b == block, 1.0, 0.0)
        send_at += here * (owner_across * cap + rank_across)
        source += jnp.where(down == wanted, block * cap + rank_down, 0.0)
    source = jnp.sum(source, axis=0, keepdims=True)
    per = CHUNK * cap
    r = iota((rows, cyc), 0)
    position = (r // per * cap + r % cap).astype(F32)
    for f in range(CHUNK):
        hit = (position == send_at) & (r % per // cap == f)
        pack[:, pl.ds(f * cyc, cyc)] = jnp.where(hit, 1.0, 0.0).astype(BF16)
    r = iota((rows, slot_dev * tile), 0)
    position = (r // per * cap + r % cap).astype(F32)
    for f in range(CHUNK):
        hit = (position == source) & (r % per // cap == f)
        pick[f] = jnp.where(hit, 1.0, 0.0).astype(BF16)

    pl.semaphore_wait(barrier, n_blk + 1)

    push_mask = remote(mask, mask_far, pm_send, pm_recv, b, c_peer)
    push_mask.start()
    push_first(0).start()
    push_first(1).start()

    @pl.loop(2, n)
    def _(h):
        push_field(h).start()

    tab_own.wait()
    tab_other.wait()
    for side_of in range(2):

        @pl.loop(0, lon // BASE)
        def _(a):
            ca = tabs[side_of, 0, pl.ds(a, 1), :]
            sa = tabs[side_of, 1, pl.ds(a, 1), :]
            cb = tabs[side_of, 2]
            sb = tabs[side_of, 3]
            at = pl.ds(pl.multiple_of(a * BASE, BASE), BASE)
            for c, value in enumerate((ca * cb - sa * sb, -(sa * cb + ca * sb))):
                high = value.astype(BF16)
                wh[side_of, at, pl.ds(c * m_dev, m_dev)] = high
                rest = value - high.astype(F32)
                wl[side_of, at, pl.ds(c * m_dev, m_dev)] = rest.astype(BF16)

    mask_own.wait()
    push_mask.wait()

    def turn(index):
        quarter = (index * iota((1, m_dev), 1)) % 4
        real = jnp.where(quarter == 0, 1.0, jnp.where(quarter == 2, -1.0, 0.0))
        imag = jnp.where(quarter == 3, 1.0, jnp.where(quarter == 1, -1.0, 0.0))
        return real, imag

    def y_copy(h):
        return remote(y_send.at[h % 2], y_recv.at[h], ys_sem.at[h % 2], yr_sem.at[h % 4], b, y_peer)

    def transform(h):
        near_copy(h).wait()

        @pl.when(h < 2)
        def _():
            push_first(h).wait()

        @pl.when(h == 0)
        def _():
            for half in (1, 0):
                for j in range(LINE):
                    leg_copy(half, j).start()

        @pl.when(h >= 2)
        def _():
            far_copy(h).wait()

        @pl.when((h >= 1) & (h + 1 < n))
        def _():
            near_copy(h + 1).start()
            push_field(h + 1).wait()
            far_copy(h + 1).start()

        @pl.when(h >= 2)
        def _():
            y_copy(h - 2).wait_send()

        for i, (data, wet) in enumerate(((near, mask_near), (far, mask_far))):
            value = (data[h % 2] * wet[...].astype(F32)[None]).reshape(rows, lon)
            high = value.astype(BF16)
            parts[pl.ds(i * rows, rows), :] = high
            rest = value - high.astype(F32)
            parts[pl.ds((2 + i) * rows, rows), :] = rest.astype(BF16)
        near_r, near_i = turn(o)
        far_r, far_i = turn(c_peer)
        for side_of in (1, 0):
            both = jnp.dot(parts[...], wh[side_of], preferred_element_type=F32)
            total = both[: 2 * rows] + both[2 * rows :]
            total += jnp.dot(
                parts[pl.ds(0, 2 * rows), :], wl[side_of], preferred_element_type=F32
            )
            nr, ni = total[:rows, :m_dev], total[:rows, m_dev:]
            fr, fi = total[rows:, :m_dev], total[rows:, m_dev:]
            real = near_r * nr - near_i * ni + far_r * fr - far_i * fi
            imag = near_r * ni + near_i * nr + far_r * fi + far_i * fr
            target = y_send if side_of else y_own
            target[h % 2, :, pl.ds(0, m_dev)] = real
            target[h % 2, :, pl.ds(m_dev, m_dev)] = imag
            if side_of:
                y_copy(h).start()

    def a_copy(h, k):
        to = (b + k) % n_blk
        return remote(
            a_send.at[h, to], a_recv.at[h, b], as_sem.at[h % 4, k - 1], ar_sem.at[h % 4, k - 1], to, o
        )

    def exchange(h):
        y_copy(h).wait_recv()
        spectrum = (y_own[h % 2] + y_recv[h]).astype(BF16)
        packed = jnp.dot(pack[...], spectrum, preferred_element_type=F32).astype(BF16)
        a_send[h] = packed.reshape(n_blk, per, 2 * m_dev)
        a_recv[h, b] = a_send[h, b]
        for k in range(1, n_blk):
            a_copy(h, k).start()

    diagonal = (iota((1, tile, slot_dev * tile), 1)) == (iota((1, tile, slot_dev * tile), 2) % tile)

    def spread_out(h):
        for k in range(1, n_blk):
            a_copy(h, k).wait()
        got = a_recv[h].reshape(rows, 2 * m_dev)
        for c in range(2):
            for f in range(CHUNK):
                value = lax.dot_general(
                    got[:, c * m_dev : (c + 1) * m_dev], pick[f],
                    (((0,), (0,)), ((), ())), preferred_element_type=F32,
                )
                value = value.reshape(groups, tile, slot_dev * tile)
                spread[:, pl.ds((f * 2 + c) * tile, tile), :] = jnp.where(
                    diagonal, value, 0.0
                ).astype(BF16)

    def x_copy(h, j):
        return remote(
            xs.at[h % 2, j], xr.at[h % 5, j], xs_sem.at[h % 2, j], xr_sem.at[h % 5, j], x_peer, o
        )

    def product(g, half, first=0, count=LINE):
        at = pl.ds(pl.multiple_of(g * tile, tile), tile)
        lanes = pl.ds(first * l_dev, count * l_dev)
        table_part = leg[half, :, at, lanes].reshape(slot_dev * tile, count * l_dev)
        return at, jnp.dot(spread[g], table_part, preferred_element_type=F32)

    def low_end_copy(h):
        return remote(
            zbs.at[h], zbr.at[h, pl.ds(0, LINE - 1)], zbs_sem.at[h % 4, 0], zbr_sem.at[h % 4, 0],
            mate * PAIR + x, o,
        )

    def low_inner_copy(h, j):
        to_z = (mate, far_end, far_inner)[j]
        return remote(
            zbs.at[h, j], zbr.at[h, (0, 1, 3)[j]], zbs_sem.at[h % 4, j],
            zbr_sem.at[h % 4, (0, 1, 1)[j]], to_z * PAIR + x, o,
        )

    def low_x_copy(h):
        return remote(xbs.at[h], xbr.at[h], xbs_sem.at[h % 4], xbr_sem.at[h % 4], x_peer, o)

    def low_part(h, j, half):
        if half == 0:
            return own_part[h % 3, j, :, pl.ds(m_x, m_dev - m_x), :]
        return far_part[h % 3, j]

    def low_middle(h):
        @pl.when(is_end == 0)
        def _():
            low_end_copy(h).wait_recv()
            for j in (1, 2):
                for half in range(2):
                    value = low_part(h, j, half) + zbr[h, j - 1, half].astype(F32)
                    zbs[h, j, half] = value.astype(BF16)
                low_inner_copy(h, j).start()

    def low_across(h):
        def add(first, second):
            for half in (1, 0):
                value = low_part(h, LINE - 1, half)
                value += zbr[h, first, half].astype(F32) + zbr[h, second, half].astype(F32)
                if half == 0:
                    own_part[h % 3, LINE - 1, :, pl.ds(m_x, m_dev - m_x), :] = value
                else:
                    xbs[h] = value.astype(BF16)
            low_x_copy(h).start()

        @pl.when(is_end == 1)
        def _():
            low_inner_copy(h, 0).wait_recv()
            low_inner_copy(h, 1).wait_recv()
            add(0, 1)

        @pl.when(is_end == 0)
        def _():
            low_inner_copy(h, 2).wait_recv()
            add(2, 3)

    def products(h):
        @pl.when(h == 0)
        def _():
            for j in range(LINE):
                leg_copy(1, j).wait()

        @pl.when(h >= 2)
        def _():
            for j in range(LINE):
                x_copy(h - 2, j).wait_send()

        def x_products(first, count):
            @pl.loop(0, x_groups)
            def _(g):
                at, value = product(g, 1, first, count)
                for j in range(count):
                    piece = value[:, j * l_dev : (j + 1) * l_dev].reshape(2 * CHUNK, tile, l_dev)
                    xs[h % 2, first + j, :, at, :] = piece.astype(BF16)

        def x_start(first, count):
            for j in range(count):
                x_copy(h, first + j).start()

        @pl.when(h == 0)
        def _():
            x_products(0, 2)
            exchange(1)
            x_start(0, 2)
            x_products(2, 2)
            x_start(2, 2)

        @pl.when(h > 0)
        def _():
            x_products(0, LINE)
            x_start(0, LINE)

        @pl.when(h == 0)
        def _():
            for j in range(LINE):
                leg_copy(0, j).wait()

        @pl.loop(x_groups, groups)
        def _(g):
            low = pl.ds(pl.multiple_of((g - x_groups) * tile, tile), tile)
            for half in range(2):
                at, value = product(g, half)
                for j in range(LINE):
                    piece = value[:, j * l_dev : (j + 1) * l_dev].reshape(2 * CHUNK, tile, l_dev)
                    if half == 0:
                        own_part[h % 3, j, :, at, :] = piece
                    else:
                        far_part[h % 3, j, :, low, :] = piece
                    if j < LINE - 1:
                        zbs[h, j, half, :, low, :] = piece.astype(BF16)

        @pl.when(is_end == 1)
        def _():
            low_end_copy(h).start()

        @pl.when(is_end == 0)
        def _():
            low_inner_copy(h, 0).start()

        @pl.loop(0, x_groups)
        def _(g):
            at, value = product(g, 0)
            for j in range(LINE):
                piece = value[:, j * l_dev : (j + 1) * l_dev].reshape(2 * CHUNK, tile, l_dev)
                own_part[h % 3, j, :, at, :] = piece

    def z_copy(h, j, to_z, slot):
        return remote(
            xr.at[h % 5, j], zr.at[h % 4, slot], zs_sem.at[h % 4, j], zr_sem.at[h % 4, slot],
            to_z * PAIR + x, o,
        )

    def end_copy(h, j):
        return z_copy(h, j, mate, j)

    def inner_copy(h, j):
        return z_copy(h, j, (mate, far_end, far_inner)[j], (0, 1, 3)[j])

    high = pl.ds(0, m_x)

    def first_sums(h):
        for j in range(LINE):
            if j == LINE - 1:

                @pl.when(h == n - 1)
                def _():
                    low_across(h)

            x_copy(h, j).wait_recv()
            value = own_part[h % 3, j, :, high, :] + xr[h % 5, j].astype(F32)
            if j == LINE - 1:
                own_part[h % 3, j, :, high, :] = value
                continue

            @pl.when(is_end == 1)
            def _():
                xr[h % 5, j] = value.astype(BF16)
                end_copy(h, j).start()

            @pl.when(is_end == 0)
            def _():
                if j == 0:
                    xr[h % 5, j] = value.astype(BF16)
                else:
                    end_copy(h, j - 1).wait_recv()
                    xr[h % 5, j] = (value + zr[h % 4, j - 1].astype(F32)).astype(BF16)
                inner_copy(h, j).start()

    def out_copy(h):
        return pltpu.make_async_copy(
            stage.at[h % 2], out.at[:, pl.ds(h * CHUNK, CHUNK)], out_sem.at[h % 2]
        )

    def last_sums(h):
        @pl.when(h >= 2)
        def _():
            out_copy(h - 2).wait()

        def add(first, second):
            value = own_part[h % 3, LINE - 1, :, high, :]
            value += zr[h % 4, first].astype(F32) + zr[h % 4, second].astype(F32)
            own_part[h % 3, LINE - 1, :, high, :] = value

        @pl.when(is_end == 1)
        def _():
            inner_copy(h, 0).wait_recv()
            inner_copy(h, 1).wait_recv()
            add(0, 1)
            for j in range(LINE - 1):
                end_copy(h, j).wait_send()
            low_end_copy(h).wait_send()

        @pl.when(is_end == 0)
        def _():
            end_copy(h, 2).wait_recv()
            inner_copy(h, 2).wait_recv()
            add(2, 3)
            for j in range(LINE - 1):
                inner_copy(h, j).wait_send()
                low_inner_copy(h, j).wait_send()

        low_x_copy(h).wait_recv()
        low = pl.ds(m_x, m_dev - m_x)
        own_part[h % 3, LINE - 1, :, low, :] += xbr[h].astype(F32)
        for f in range(CHUNK):
            for c in range(2):
                stage[h % 2, :, f, c, :] = own_part[h % 3, LINE - 1, 2 * f + c].T
        low_x_copy(h).wait_send()
        out_copy(h).start()

    @pl.loop(0, n + 5)
    def _(t):
        def when(step, delay):
            @pl.when((t >= delay) & (t < n + delay))
            def _():
                step(t - delay)

        when(last_sums, 5)

        @pl.when((t >= 4) & (t < n + 3))
        def _():
            low_across(t - 4)

        when(transform, 0)

        @pl.when((t >= 1) & (t != 2) & (t < n + 1))
        def _():
            exchange(t - 1)

        when(spread_out, 2)
        when(products, 2)
        when(low_middle, 3)
        when(first_sums, 3)

    for h in (n - 2, n - 1):
        y_copy(h).wait_send()
        out_copy(h).wait()
        for j in range(LINE):
            x_copy(h, j).wait_send()


def fused_body(field, ocean_mask, plan, legendre):
    fields, cyc, lon = field.shape
    slot_dev, m_dev, degrees = legendre.shape
    n_blk = LINE * PAIR
    l_dev = degrees // n_blk
    tile = 16
    groups = m_dev // tile
    n = fields // CHUNK
    rows = CHUNK * cyc
    cap = (cyc + n_blk - 1) // n_blk
    per = CHUNK * cap
    table = jnp.asarray(table_of(lon, m_dev))
    x_groups = groups - max(groups // 8, 1)
    piece = (2 * CHUNK, m_dev, l_dev)
    high = (2 * CHUNK, x_groups * tile, l_dev)
    low = (2 * CHUNK, m_dev - x_groups * tile, l_dev)
    dma = pltpu.SemaphoreType.DMA
    any_spec = pl.BlockSpec(memory_space=pl.ANY)
    vmem_spec = pl.BlockSpec(memory_space=pltpu.VMEM)
    scratch = [
        pltpu.VMEM((2, slot_dev, m_dev, LINE * l_dev), BF16),
        pltpu.VMEM((groups, 2 * CHUNK * tile, slot_dev * tile), BF16),
        pltpu.VMEM((3, LINE) + piece, F32),
        pltpu.VMEM((3, LINE) + low, F32),
        pltpu.VMEM((2, LINE) + high, BF16),
        pltpu.VMEM((5, LINE) + high, BF16),
        pltpu.VMEM((4, 4) + high, BF16),
        pltpu.VMEM((n, LINE - 1, 2) + low, BF16),
        pltpu.VMEM((n, 4, 2) + low, BF16),
        pltpu.VMEM((n,) + low, BF16),
        pltpu.VMEM((n,) + low, BF16),
        pltpu.VMEM((2, lon, 2 * m_dev), BF16),
        pltpu.VMEM((2, lon, 2 * m_dev), BF16),
        pltpu.VMEM((2, CHUNK, cyc, lon), F32),
        pltpu.VMEM((2, CHUNK, cyc, lon), F32),
        pltpu.VMEM((cyc, lon), jnp.int32),
        pltpu.VMEM((cyc, lon), jnp.int32),
        pltpu.VMEM((4 * rows, lon), BF16),
        pltpu.VMEM((2, rows, 2 * m_dev), F32),
        pltpu.VMEM((2, rows, 2 * m_dev), F32),
        pltpu.VMEM((n, rows, 2 * m_dev), F32),
        pltpu.VMEM((n, n_blk, per, 2 * m_dev), BF16),
        pltpu.VMEM((n, n_blk, per, 2 * m_dev), BF16),
        pltpu.VMEM((CHUNK, rows, slot_dev * tile), BF16),
        pltpu.VMEM((rows, rows), BF16),
        pltpu.VMEM((2, l_dev, CHUNK, 2, m_dev), F32),
        pltpu.VMEM((2, 4, BASE, m_dev), F32),
        dma((2, LINE)),
        dma((2,)),
        dma((2,)),
        dma,
        dma((2,)),
        dma((2,)),
        dma((n,)), dma((n,)),
        dma, dma,
        dma((2,)), dma((4,)),
        dma((4, n_blk - 1)), dma((4, n_blk - 1)),
        dma((2, LINE)), dma((5, LINE)),
        dma((4, 3)), dma((4, 4)),
        dma((4, 3)), dma((4, 2)),
        dma((4,)), dma((4,)),
    ]
    dims = (n, groups, x_groups, tile, m_dev, l_dev, cyc, lon, slot_dev, cap)
    sums, _ = pl.pallas_call(
        functools.partial(fused_kernel, dims),
        out_shape=[
            jax.ShapeDtypeStruct((l_dev, fields, 2, m_dev), F32),
            jax.ShapeDtypeStruct(field.shape, F32),
        ],
        in_specs=[any_spec] * 4 + [vmem_spec],
        out_specs=[any_spec] * 2,
        scratch_shapes=scratch,
        compiler_params=pltpu.CompilerParams(
            collective_id=0, has_side_effects=True, vmem_limit_bytes=66 * 1000 * 1000
        ),
        name="analysis",
    )(field, ocean_mask, legendre, table, plan.reshape(1, -1))
    parts = 8
    return pl.pallas_call(
        hand_on_kernel,
        out_shape=jax.ShapeDtypeStruct(sums.shape, F32),
        in_specs=[any_spec],
        out_specs=any_spec,
        scratch_shapes=[
            pltpu.VMEM((parts, l_dev // parts) + sums.shape[1:], F32),
            dma((parts,)), dma((parts,)),
        ],
        name="hand_on",
    )(sums)


def hand_on_kernel(source, target, held, in_sem, out_sem):
    parts, depth = held.shape[:2]

    def into(k):
        return pltpu.make_async_copy(source.at[pl.ds(k * depth, depth)], held.at[k], in_sem.at[k])

    def away(k):
        return pltpu.make_async_copy(held.at[k], target.at[pl.ds(k * depth, depth)], out_sem.at[k])

    for k in range(parts):
        into(k).start()
    for k in range(parts):
        into(k).wait()
        away(k).start()
    for k in range(parts):
        away(k).wait()


def fits(mesh, field, legendre):
    shape = dict(mesh.shape)
    n_blk, n_order = shape["blk"], shape["order"]
    cyc, lon = field.shape[1] // n_blk, field.shape[2] // n_order
    slots, m_dev = legendre.shape[0] // n_blk, legendre.shape[1] // n_order
    return (
        n_blk == LINE * PAIR
        and n_order == 4
        and field.shape[0] % CHUNK == 0
        and field.shape[0] // CHUNK >= 5
        and lon == BASE * BASE
        and NLON == 4 * lon
        and m_dev % 128 == 0
        and legendre.shape[2] == n_blk * 128
        and cyc % n_blk == 0
        and slots % 8 == 0
    )


def twiddle(first, count):
    longitudes = first + jnp.arange(count, dtype=jnp.int32)
    orders = jnp.arange(M, dtype=jnp.int32)
    product = longitudes[:, None] * orders[None, :] % NLON
    angle = product.astype(jnp.float32) * (2.0 * math.pi / NLON)
    scale = 1.0 / math.sqrt(NLON)
    return jnp.stack([jnp.cos(angle) * scale, -jnp.sin(angle) * scale], axis=1)


def transform(values, table):
    return jnp.einsum("frn,ncm->frcm", values, table, precision=lax.Precision.HIGHEST)


def pack_cycles(masked, plan, slot_dev):
    n_blk = lax.axis_size("blk")
    own_index = lax.axis_index("blk")
    cycle_dev = masked.shape[1]
    cap = (cycle_dev + n_blk - 1) // n_blk
    grid = plan.reshape(n_blk, cycle_dev)
    owner = grid // slot_dev
    positions = jnp.arange(cycle_dev, dtype=jnp.int32)
    earlier = positions[None, :] < positions[:, None]
    same_owner = owner[:, :, None] == owner[:, None, :]
    rank = jnp.sum(same_owner & earlier[None], axis=2, dtype=jnp.int32)
    send_pos = owner * cap + rank
    local_pos = lax.dynamic_index_in_dim(send_pos, own_index, 0, keepdims=False)
    buffer_ids = jnp.arange(n_blk * cap, dtype=jnp.int32)
    send_onehot = (buffer_ids[:, None] == local_pos[None, :]).astype(jnp.float32)
    outgoing = jnp.einsum("qr,frn->fqn", send_onehot, masked, precision=lax.Precision.HIGHEST)
    arrived = lax.all_to_all(outgoing, "blk", split_axis=1, concat_axis=1, tiled=True)
    source_pos = (jnp.arange(n_blk, dtype=jnp.int32)[:, None] * cap + rank).reshape(-1)
    mine = (owner == own_index).reshape(-1)
    slot_local = (grid % slot_dev).reshape(-1)
    slot_ids = jnp.arange(slot_dev, dtype=jnp.int32)
    slot_onehot = ((slot_local[None, :] == slot_ids[:, None]) & mine[None, :]).astype(jnp.float32)
    source_onehot = (source_pos[:, None] == buffer_ids[None, :]).astype(jnp.float32)
    receive_map = jnp.dot(slot_onehot, source_onehot, precision=lax.Precision.HIGHEST)
    return jnp.einsum("pq,fqn->fpn", receive_map, arrived, precision=lax.Precision.HIGHEST)


def degree_sums(legendre, spectrum):
    n_blk = lax.axis_size("blk")
    own_index = lax.axis_index("blk")
    pairs = n_blk // 2
    degree_dev = legendre.shape[2] // n_blk
    own_pair, own_side = own_index // 2, own_index % 2
    swap = [(i, i + 1 - 2 * (i % 2)) for i in range(n_blk)]

    def terms_for(target):
        table = lax.dynamic_slice_in_dim(legendre, target * degree_dev, degree_dev, 2)
        return jnp.einsum("pml,fpcm->lfcm", table, spectrum, preferred_element_type=jnp.float32)

    def pair_sum(step):
        base = (own_pair + step) % pairs * 2
        given = terms_for(base + 1 - own_side).astype(jnp.bfloat16)
        taken = lax.ppermute(given, "blk", swap)
        return terms_for(base + own_side) + taken.astype(jnp.float32)

    steps = sorted(range(1, pairs), key=lambda step: abs(2 * step - pairs))
    arrived = []
    for step in steps:
        shift = [(i, (i + 2 * step) % n_blk) for i in range(n_blk)]
        arrived.append(lax.ppermute(pair_sum(step).astype(jnp.bfloat16), "blk", shift))
    total = pair_sum(0)
    for piece in arrived:
        total = total + piece.astype(jnp.float32)
    return total


def body(field, ocean_mask, plan, legendre):
    lon_local = field.shape[2]
    slot_dev = legendre.shape[0]
    masked = field * ocean_mask.astype(jnp.float32)[None]
    packed = pack_cycles(masked, plan, slot_dev)
    first = lax.axis_index("order") * lon_local
    terms = transform(packed, twiddle(first, lon_local))
    spectrum = lax.psum_scatter(terms, "order", scatter_dimension=3, tiled=True).astype(
        jnp.bfloat16
    )
    coefficients = degree_sums(legendre, spectrum)
    return coefficients


def solution(mesh):
    placed = (P(None, "blk", "order"), P("blk", "order"), P(), P("blk", "order", None))

    def run(field, ocean_mask, plan, legendre):
        chosen = fused_body if fits(mesh, field, legendre) else body
        mapped = jax.shard_map(
            chosen, mesh=mesh, in_specs=placed, out_specs=P("blk", None, None, "order"),
            check_vma=False,
        )
        return mapped(field, ocean_mask, plan, legendre)

    return run
```

```python
import functools
import math

import jax
import jax.numpy as jnp
import numpy as np
from jax import lax
from jax.experimental import pallas as pl
from jax.experimental.pallas import tpu as pltpu
from jax.sharding import PartitionSpec as P

NLON = 4096
M = 1024
MESH = pl.DeviceIdType.MESH
F32, BF16 = jnp.float32, jnp.bfloat16

LINE, PAIR = 4, 2
CHUNK = 2
BASE = 32


def table_of(lon_local, orders):
    coarse = np.arange(lon_local // BASE)[:, None] * BASE
    fine = np.arange(BASE)[:, None]
    m = np.arange(M)[None, :]

    def parts(n, scale):
        angle = (n * m % NLON) * (2.0 * math.pi / NLON)
        return [np.cos(angle) * scale, np.sin(angle) * scale]

    both = parts(coarse, 1.0) + parts(fine, 1.0 / math.sqrt(NLON))
    owners = M // orders
    stacked = np.stack([t.reshape(BASE, owners, orders) for t in both])
    return stacked.transpose(2, 0, 1, 3).astype(np.float32)


def fused_kernel(
    dims,
    field, mask, legendre, table, plan,
    out, far_field,
    leg, spread, own_part, far_part, xs, xr, zr, zbs, zbr, xbs, xbr, wh, wl, near, far, mask_near, mask_far, parts,
    y_own, y_send, y_recv, y_first, y_begun, a_send, a_recv, pick, pack, stage, tabs,
    leg_sem, near_sem, far_sem, mask_sem, tab_sem, out_sem,
    pf_send, pf_recv, pm_send, pm_recv, ys_sem, yr_sem, as_sem, ar_sem,
    xs_sem, xr_sem, zs_sem, zr_sem, zbs_sem, zbr_sem, xbs_sem, xbr_sem, yf_sem, yb_sem,
):
    n, groups, x_groups, tile, m_dev, l_dev, cyc, lon, slot_dev, cap = dims
    m_x = x_groups * tile
    rows = CHUNK * cyc
    n_blk = LINE * PAIR
    b = lax.axis_index("blk")
    o = lax.axis_index("order")
    z, x = b // PAIR, b % PAIR
    side = z // 2
    odd = z % 2
    is_end = 1 - (odd + side - 2 * odd * side)
    far_end = (LINE - 1) * (1 - side)
    far_inner = 2 - side
    mate = 2 * side + 1 - odd
    dest = [
        is_end * far_end + (1 - is_end) * mate,
        is_end * far_inner + (1 - is_end) * far_end,
        is_end * mate + (1 - is_end) * far_inner,
        z,
    ]
    x_peer = b + 1 - 2 * x
    y_peer = (o + 2) % 4
    c_peer = o + 1 - 2 * (o % 2)

    def remote(src, dst, send, recv, blk, order):
        return pltpu.make_async_remote_copy(
            src_ref=src, dst_ref=dst, send_sem=send, recv_sem=recv,
            device_id=(blk, order), device_id_type=MESH,
        )

    def leg_copy(half, j):
        block = dest[j] * PAIR + (x if half == 0 else 1 - x)
        lanes = pl.ds(pl.multiple_of(block * l_dev, l_dev), l_dev)
        return pltpu.make_async_copy(
            legendre.at[:, :, lanes],
            leg.at[half, :, :, pl.ds(j * l_dev, l_dev)],
            leg_sem.at[half, j],
        )

    def near_copy(h):
        return pltpu.make_async_copy(
            field.at[pl.ds(h * CHUNK, CHUNK)], near.at[h % 2], near_sem.at[h % 2]
        )

    def far_copy(h):
        return pltpu.make_async_copy(
            far_field.at[pl.ds(h * CHUNK, CHUNK)], far.at[h % 2], far_sem.at[h % 2]
        )

    def push_field(h):
        fields = pl.ds(h * CHUNK, CHUNK)
        return remote(
            field.at[fields], far_field.at[fields], pf_send.at[h], pf_recv.at[h], b, c_peer
        )

    def push_first(h):
        return remote(
            field.at[pl.ds(h * CHUNK, CHUNK)], far.at[h], pf_send.at[h], pf_recv.at[h], b, c_peer
        )

    tab_own = pltpu.make_async_copy(table.at[o], tabs.at[0], tab_sem.at[0])
    tab_other = pltpu.make_async_copy(table.at[y_peer], tabs.at[1], tab_sem.at[1])
    tab_own.start()
    tab_other.start()
    mask_own = pltpu.make_async_copy(mask, mask_near, mask_sem)
    mask_own.start()
    near_copy(0).start()
    near_copy(1).start()

    barrier = pltpu.get_barrier_semaphore()
    for k in range(1, n_blk):
        pl.semaphore_signal(barrier, inc=1, device_id=((b + k) % n_blk, o), device_id_type=MESH)
    pl.semaphore_signal(barrier, inc=1, device_id=(b, y_peer), device_id_type=MESH)
    pl.semaphore_signal(barrier, inc=1, device_id=(b, c_peer), device_id_type=MESH)

    def iota(shape, axis):
        return lax.broadcasted_iota(jnp.int32, shape, axis)

    wanted = (b * slot_dev + iota((1, slot_dev * tile), 1) // tile).astype(F32)
    row_id, col_id = iota((cyc, cyc), 0), iota((cyc, cyc), 1)
    send_at = jnp.zeros((1, cyc), F32)
    source = jnp.zeros((cyc, slot_dev * tile), F32)
    for block in range(n_blk):
        across = plan[:, pl.ds(block * cyc, cyc)].astype(F32)
        down = jnp.sum(jnp.where(row_id == col_id, across, 0.0), axis=1, keepdims=True)
        owner_across = jnp.floor((across + 0.5) * (1.0 / slot_dev))
        owner_down = jnp.floor((down + 0.5) * (1.0 / slot_dev))
        same = owner_down == owner_across
        rank_across = jnp.sum(
            jnp.where(same & (row_id < col_id), 1.0, 0.0), axis=0, keepdims=True
        )
        rank_down = jnp.sum(
            jnp.where(same & (col_id < row_id), 1.0, 0.0), axis=1, keepdims=True
        )
        here = jnp.where(b == block, 1.0, 0.0)
        send_at += here * (owner_across * cap + rank_across)
        source += jnp.where(down == wanted, block * cap + rank_down, 0.0)
    source = jnp.sum(source, axis=0, keepdims=True)
    per = CHUNK * cap
    r = iota((rows, cyc), 0)
    position = (r // per * cap + r % cap).astype(F32)
    for f in range(CHUNK):
        hit = (position == send_at) & (r % per // cap == f)
        pack[:, pl.ds(f * cyc, cyc)] = jnp.where(hit, 1.0, 0.0).astype(BF16)
    r = iota((rows, slot_dev * tile), 0)
    position = (r // per * cap + r % cap).astype(F32)
    for f in range(CHUNK):
        hit = (position == source) & (r % per // cap == f)
        pick[f] = jnp.where(hit, 1.0, 0.0).astype(BF16)

    pl.semaphore_wait(barrier, n_blk + 1)

    push_mask = remote(mask, mask_far, pm_send, pm_recv, b, c_peer)
    push_mask.start()
    push_first(0).start()
    push_first(1).start()

    @pl.loop(2, n)
    def _(h):
        push_field(h).start()

    tab_own.wait()
    tab_other.wait()
    for side_of in range(2):

        @pl.loop(0, lon // BASE)
        def _(a):
            ca = tabs[side_of, 0, pl.ds(a, 1), :]
            sa = tabs[side_of, 1, pl.ds(a, 1), :]
            cb = tabs[side_of, 2]
            sb = tabs[side_of, 3]
            at = pl.ds(pl.multiple_of(a * BASE, BASE), BASE)
            for c, value in enumerate((ca * cb - sa * sb, -(sa * cb + ca * sb))):
                high = value.astype(BF16)
                wh[side_of, at, pl.ds(c * m_dev, m_dev)] = high
                rest = value - high.astype(F32)
                wl[side_of, at, pl.ds(c * m_dev, m_dev)] = rest.astype(BF16)

    mask_own.wait()
    push_mask.wait()

    def turn(index):
        quarter = (index * iota((1, m_dev), 1)) % 4
        real = jnp.where(quarter == 0, 1.0, jnp.where(quarter == 2, -1.0, 0.0))
        imag = jnp.where(quarter == 3, 1.0, jnp.where(quarter == 1, -1.0, 0.0))
        return real, imag

    def y_copy(h):
        return remote(y_send.at[h % 2], y_recv.at[h], ys_sem.at[h % 2], yr_sem.at[h % 4], b, y_peer)

    first_y = remote(y_first, y_begun, yf_sem, yb_sem, b, y_peer)

    def transform(h):
        near_copy(h).wait()

        @pl.when(h < 2)
        def _():
            push_first(h).wait()

        @pl.when(h == 0)
        def _():
            for j in range(LINE):
                leg_copy(1, j).start()

        @pl.when(h >= 2)
        def _():
            far_copy(h).wait()

        @pl.when((h >= 1) & (h + 1 < n))
        def _():
            near_copy(h + 1).start()
            push_field(h + 1).wait()
            far_copy(h + 1).start()

        @pl.when(h == 1)
        def _():
            for j in range(LINE):
                leg_copy(0, j).start()

        @pl.when(h >= 3)
        def _():
            y_copy(h - 2).wait_send()

        for i, (data, wet) in enumerate(((near, mask_near), (far, mask_far))):
            value = (data[h % 2] * wet[...].astype(F32)[None]).reshape(rows, lon)
            high = value.astype(BF16)
            parts[pl.ds(i * rows, rows), :] = high
            rest = value - high.astype(F32)
            parts[pl.ds((2 + i) * rows, rows), :] = rest.astype(BF16)
        near_r, near_i = turn(o)
        far_r, far_i = turn(c_peer)
        for side_of in (1, 0):
            both = jnp.dot(parts[...], wh[side_of], preferred_element_type=F32)
            total = both[: 2 * rows] + both[2 * rows :]
            total += jnp.dot(
                parts[pl.ds(0, 2 * rows), :], wl[side_of], preferred_element_type=F32
            )
            nr, ni = total[:rows, :m_dev], total[:rows, m_dev:]
            fr, fi = total[rows:, :m_dev], total[rows:, m_dev:]
            real = near_r * nr - near_i * ni + far_r * fr - far_i * fi
            imag = near_r * ni + near_i * nr + far_r * fi + far_i * fr
            if side_of:

                @pl.when(h == 0)
                def _():
                    y_first[:, pl.ds(0, m_dev)] = real.astype(BF16)
                    y_first[:, pl.ds(m_dev, m_dev)] = imag.astype(BF16)
                    first_y.start()

                @pl.when(h > 0)
                def _():
                    y_send[h % 2, :, pl.ds(0, m_dev)] = real
                    y_send[h % 2, :, pl.ds(m_dev, m_dev)] = imag
                    y_copy(h).start()

            else:
                y_own[h % 2, :, pl.ds(0, m_dev)] = real
                y_own[h % 2, :, pl.ds(m_dev, m_dev)] = imag

    def a_copy(h, k):
        to = (b + k) % n_blk
        return remote(
            a_send.at[h, to], a_recv.at[h, b], as_sem.at[h % 4, k - 1], ar_sem.at[h % 4, k - 1], to, o
        )

    def exchange(h):
        @pl.when(h == 0)
        def _():
            first_y.wait()
            y_recv[h] = y_begun[...].astype(F32)

        @pl.when(h > 0)
        def _():
            y_copy(h).wait_recv()

        spectrum = (y_own[h % 2] + y_recv[h]).astype(BF16)
        packed = jnp.dot(pack[...], spectrum, preferred_element_type=F32).astype(BF16)
        a_send[h] = packed.reshape(n_blk, per, 2 * m_dev)
        a_recv[h, b] = a_send[h, b]
        for k in range(1, n_blk):
            a_copy(h, k).start()

    diagonal = (iota((1, tile, slot_dev * tile), 1)) == (iota((1, tile, slot_dev * tile), 2) % tile)

    def spread_out(h):
        for k in range(1, n_blk):
            a_copy(h, k).wait()
        got = a_recv[h].reshape(rows, 2 * m_dev)
        for c in range(2):
            for f in range(CHUNK):
                value = lax.dot_general(
                    got[:, c * m_dev : (c + 1) * m_dev], pick[f],
                    (((0,), (0,)), ((), ())), preferred_element_type=F32,
                )
                value = value.reshape(groups, tile, slot_dev * tile)
                spread[:, pl.ds((f * 2 + c) * tile, tile), :] = jnp.where(
                    diagonal, value, 0.0
                ).astype(BF16)

    def x_copy(h, j):
        return remote(
            xs.at[h % 2, j], xr.at[h % 5, j], xs_sem.at[h % 2, j], xr_sem.at[h % 5, j], x_peer, o
        )

    def product(g, half, first=0, count=LINE):
        at = pl.ds(pl.multiple_of(g * tile, tile), tile)
        lanes = pl.ds(first * l_dev, count * l_dev)
        table_part = leg[half, :, at, lanes].reshape(slot_dev * tile, count * l_dev)
        return at, jnp.dot(spread[g], table_part, preferred_element_type=F32)

    def low_end_copy(h):
        return remote(
            zbs.at[h], zbr.at[h, pl.ds(0, LINE - 1)], zbs_sem.at[h % 4, 0], zbr_sem.at[h % 4, 0],
            mate * PAIR + x, o,
        )

    def low_inner_copy(h, j):
        to_z = (mate, far_end, far_inner)[j]
        return remote(
            zbs.at[h, j], zbr.at[h, (0, 1, 3)[j]], zbs_sem.at[h % 4, j],
            zbr_sem.at[h % 4, (0, 1, 1)[j]], to_z * PAIR + x, o,
        )

    def low_x_copy(h):
        return remote(xbs.at[h], xbr.at[h], xbs_sem.at[h % 4], xbr_sem.at[h % 4], x_peer, o)

    def low_part(h, j, half):
        if half == 0:
            return own_part[h % 3, j, :, pl.ds(m_x, m_dev - m_x), :]
        return far_part[h % 3, j]

    def low_middle(h):
        @pl.when(is_end == 0)
        def _():
            low_end_copy(h).wait_recv()
            for j in (1, 2):
                for half in range(2):
                    value = low_part(h, j, half) + zbr[h, j - 1, half].astype(F32)
                    zbs[h, j, half] = value.astype(BF16)
                low_inner_copy(h, j).start()

    def low_across(h):
        def add(first, second):
            for half in (1, 0):
                value = low_part(h, LINE - 1, half)
                value += zbr[h, first, half].astype(F32) + zbr[h, second, half].astype(F32)
                if half == 0:
                    own_part[h % 3, LINE - 1, :, pl.ds(m_x, m_dev - m_x), :] = value
                else:
                    xbs[h] = value.astype(BF16)
            low_x_copy(h).start()

        @pl.when(is_end == 1)
        def _():
            low_inner_copy(h, 0).wait_recv()
            low_inner_copy(h, 1).wait_recv()
            add(0, 1)

        @pl.when(is_end == 0)
        def _():
            low_inner_copy(h, 2).wait_recv()
            add(2, 3)

    def products(h):
        @pl.when(h == 0)
        def _():
            for j in range(LINE):
                leg_copy(1, j).wait()

        @pl.when(h >= 2)
        def _():
            for j in range(LINE):
                x_copy(h - 2, j).wait_send()

        def x_products(first, count):
            @pl.loop(0, x_groups)
            def _(g):
                at, value = product(g, 1, first, count)
                for j in range(count):
                    piece = value[:, j * l_dev : (j + 1) * l_dev].reshape(2 * CHUNK, tile, l_dev)
                    xs[h % 2, first + j, :, at, :] = piece.astype(BF16)

        def x_start(first, count):
            for j in range(count):
                x_copy(h, first + j).start()

        @pl.when(h == 0)
        def _():
            x_products(0, 2)
            exchange(1)
            x_start(0, 2)
            x_products(2, 2)
            x_start(2, 2)

        @pl.when(h > 0)
        def _():
            x_products(0, LINE)
            x_start(0, LINE)

        @pl.when(h == 0)
        def _():
            for j in range(LINE):
                leg_copy(0, j).wait()

        @pl.loop(x_groups, groups)
        def _(g):
            low = pl.ds(pl.multiple_of((g - x_groups) * tile, tile), tile)
            for half in range(2):
                at, value = product(g, half)
                for j in range(LINE):
                    piece = value[:, j * l_dev : (j + 1) * l_dev].reshape(2 * CHUNK, tile, l_dev)
                    if half == 0:
                        own_part[h % 3, j, :, at, :] = piece
                    else:
                        far_part[h % 3, j, :, low, :] = piece
                    if j < LINE - 1:
                        zbs[h, j, half, :, low, :] = piece.astype(BF16)

        @pl.when(is_end == 1)
        def _():
            low_end_copy(h).start()

        @pl.when(is_end == 0)
        def _():
            low_inner_copy(h, 0).start()

        @pl.loop(0, x_groups)
        def _(g):
            at, value = product(g, 0)
            for j in range(LINE):
                piece = value[:, j * l_dev : (j + 1) * l_dev].reshape(2 * CHUNK, tile, l_dev)
                own_part[h % 3, j, :, at, :] = piece

    def z_copy(h, j, to_z, slot):
        return remote(
            xr.at[h % 5, j], zr.at[h % 4, slot], zs_sem.at[h % 4, j], zr_sem.at[h % 4, slot],
            to_z * PAIR + x, o,
        )

    def end_copy(h, j):
        return z_copy(h, j, mate, j)

    def inner_copy(h, j):
        return z_copy(h, j, (mate, far_end, far_inner)[j], (0, 1, 3)[j])

    high = pl.ds(0, m_x)

    def first_sums(h):
        for j in range(LINE):
            if j == LINE - 1:

                @pl.when(h == n - 1)
                def _():
                    low_across(h)

            x_copy(h, j).wait_recv()
            value = own_part[h % 3, j, :, high, :] + xr[h % 5, j].astype(F32)
            if j == LINE - 1:
                own_part[h % 3, j, :, high, :] = value
                continue

            @pl.when(is_end == 1)
            def _():
                xr[h % 5, j] = value.astype(BF16)
                end_copy(h, j).start()

            @pl.when(is_end == 0)
            def _():
                if j == 0:
                    xr[h % 5, j] = value.astype(BF16)
                else:
                    end_copy(h, j - 1).wait_recv()
                    xr[h % 5, j] = (value + zr[h % 4, j - 1].astype(F32)).astype(BF16)
                inner_copy(h, j).start()

    def out_copy(h):
        return pltpu.make_async_copy(
            stage.at[h % 2], out.at[:, pl.ds(h * CHUNK, CHUNK)], out_sem.at[h % 2]
        )

    def last_sums(h):
        @pl.when(h >= 2)
        def _():
            out_copy(h - 2).wait()

        def add(first, second):
            value = own_part[h % 3, LINE - 1, :, high, :]
            value += zr[h % 4, first].astype(F32) + zr[h % 4, second].astype(F32)
            own_part[h % 3, LINE - 1, :, high, :] = value

        @pl.when(is_end == 1)
        def _():
            inner_copy(h, 0).wait_recv()
            inner_copy(h, 1).wait_recv()
            add(0, 1)
            for j in range(LINE - 1):
                end_copy(h, j).wait_send()
            low_end_copy(h).wait_send()

        @pl.when(is_end == 0)
        def _():
            end_copy(h, 2).wait_recv()
            inner_copy(h, 2).wait_recv()
            add(2, 3)
            for j in range(LINE - 1):
                inner_copy(h, j).wait_send()
                low_inner_copy(h, j).wait_send()

        low_x_copy(h).wait_recv()
        low = pl.ds(m_x, m_dev - m_x)
        own_part[h % 3, LINE - 1, :, low, :] += xbr[h].astype(F32)
        for f in range(CHUNK):
            for c in range(2):
                stage[h % 2, :, f, c, :] = own_part[h % 3, LINE - 1, 2 * f + c].T
        low_x_copy(h).wait_send()
        out_copy(h).start()

    @pl.loop(0, n + 5)
    def _(t):
        def when(step, delay):
            @pl.when((t >= delay) & (t < n + delay))
            def _():
                step(t - delay)

        when(last_sums, 5)

        @pl.when((t >= 4) & (t < n + 3))
        def _():
            low_across(t - 4)

        when(transform, 0)

        @pl.when((t >= 1) & (t != 2) & (t < n + 1))
        def _():
            exchange(t - 1)

        when(spread_out, 2)
        when(products, 2)
        when(low_middle, 3)
        when(first_sums, 3)

    for h in (n - 2, n - 1):
        y_copy(h).wait_send()
        out_copy(h).wait()
        for j in range(LINE):
            x_copy(h, j).wait_send()


def fused_body(field, ocean_mask, plan, legendre):
    fields, cyc, lon = field.shape
    slot_dev, m_dev, degrees = legendre.shape
    n_blk = LINE * PAIR
    l_dev = degrees // n_blk
    tile = 16
    groups = m_dev // tile
    n = fields // CHUNK
    rows = CHUNK * cyc
    cap = (cyc + n_blk - 1) // n_blk
    per = CHUNK * cap
    table = jnp.asarray(table_of(lon, m_dev))
    x_groups = groups - max(groups // 8, 1)
    piece = (2 * CHUNK, m_dev, l_dev)
    high = (2 * CHUNK, x_groups * tile, l_dev)
    low = (2 * CHUNK, m_dev - x_groups * tile, l_dev)
    dma = pltpu.SemaphoreType.DMA
    any_spec = pl.BlockSpec(memory_space=pl.ANY)
    vmem_spec = pl.BlockSpec(memory_space=pltpu.VMEM)
    scratch = [
        pltpu.VMEM((2, slot_dev, m_dev, LINE * l_dev), BF16),
        pltpu.VMEM((groups, 2 * CHUNK * tile, slot_dev * tile), BF16),
        pltpu.VMEM((3, LINE) + piece, F32),
        pltpu.VMEM((3, LINE) + low, F32),
        pltpu.VMEM((2, LINE) + high, BF16),
        pltpu.VMEM((5, LINE) + high, BF16),
        pltpu.VMEM((4, 4) + high, BF16),
        pltpu.VMEM((n, LINE - 1, 2) + low, BF16),
        pltpu.VMEM((n, 4, 2) + low, BF16),
        pltpu.VMEM((n,) + low, BF16),
        pltpu.VMEM((n,) + low, BF16),
        pltpu.VMEM((2, lon, 2 * m_dev), BF16),
        pltpu.VMEM((2, lon, 2 * m_dev), BF16),
        pltpu.VMEM((2, CHUNK, cyc, lon), F32),
        pltpu.VMEM((2, CHUNK, cyc, lon), F32),
        pltpu.VMEM((cyc, lon), jnp.int32),
        pltpu.VMEM((cyc, lon), jnp.int32),
        pltpu.VMEM((4 * rows, lon), BF16),
        pltpu.VMEM((2, rows, 2 * m_dev), F32),
        pltpu.VMEM((2, rows, 2 * m_dev), F32),
        pltpu.VMEM((n, rows, 2 * m_dev), F32),
        pltpu.VMEM((rows, 2 * m_dev), BF16),
        pltpu.VMEM((rows, 2 * m_dev), BF16),
        pltpu.VMEM((n, n_blk, per, 2 * m_dev), BF16),
        pltpu.VMEM((n, n_blk, per, 2 * m_dev), BF16),
        pltpu.VMEM((CHUNK, rows, slot_dev * tile), BF16),
        pltpu.VMEM((rows, rows), BF16),
        pltpu.VMEM((2, l_dev, CHUNK, 2, m_dev), F32),
        pltpu.VMEM((2, 4, BASE, m_dev), F32),
        dma((2, LINE)),
        dma((2,)),
        dma((2,)),
        dma,
        dma((2,)),
        dma((2,)),
        dma((n,)), dma((n,)),
        dma, dma,
        dma((2,)), dma((4,)),
        dma((4, n_blk - 1)), dma((4, n_blk - 1)),
        dma((2, LINE)), dma((5, LINE)),
        dma((4, 3)), dma((4, 4)),
        dma((4, 3)), dma((4, 2)),
        dma((4,)), dma((4,)),
        dma, dma,
    ]
    dims = (n, groups, x_groups, tile, m_dev, l_dev, cyc, lon, slot_dev, cap)
    sums, _ = pl.pallas_call(
        functools.partial(fused_kernel, dims),
        out_shape=[
            jax.ShapeDtypeStruct((l_dev, fields, 2, m_dev), F32),
            jax.ShapeDtypeStruct(field.shape, F32),
        ],
        in_specs=[any_spec] * 4 + [vmem_spec],
        out_specs=[any_spec] * 2,
        scratch_shapes=scratch,
        compiler_params=pltpu.CompilerParams(
            collective_id=0, has_side_effects=True, vmem_limit_bytes=66 * 1000 * 1000
        ),
        name="analysis",
    )(field, ocean_mask, legendre, table, plan.reshape(1, -1))
    parts = 8
    return pl.pallas_call(
        hand_on_kernel,
        out_shape=jax.ShapeDtypeStruct(sums.shape, F32),
        in_specs=[any_spec],
        out_specs=any_spec,
        scratch_shapes=[
            pltpu.VMEM((parts, l_dev // parts) + sums.shape[1:], F32),
            dma((parts,)), dma((parts,)),
        ],
        name="hand_on",
    )(sums)


def hand_on_kernel(source, target, held, in_sem, out_sem):
    parts, depth = held.shape[:2]

    def into(k):
        return pltpu.make_async_copy(source.at[pl.ds(k * depth, depth)], held.at[k], in_sem.at[k])

    def away(k):
        return pltpu.make_async_copy(held.at[k], target.at[pl.ds(k * depth, depth)], out_sem.at[k])

    for k in range(parts):
        into(k).start()
    for k in range(parts):
        into(k).wait()
        away(k).start()
    for k in range(parts):
        away(k).wait()


def fits(mesh, field, legendre):
    shape = dict(mesh.shape)
    n_blk, n_order = shape["blk"], shape["order"]
    cyc, lon = field.shape[1] // n_blk, field.shape[2] // n_order
    slots, m_dev = legendre.shape[0] // n_blk, legendre.shape[1] // n_order
    return (
        n_blk == LINE * PAIR
        and n_order == 4
        and field.shape[0] % CHUNK == 0
        and field.shape[0] // CHUNK >= 5
        and lon == BASE * BASE
        and NLON == 4 * lon
        and m_dev % 128 == 0
        and legendre.shape[2] == n_blk * 128
        and cyc % n_blk == 0
        and slots % 8 == 0
    )


def twiddle(first, count):
    longitudes = first + jnp.arange(count, dtype=jnp.int32)
    orders = jnp.arange(M, dtype=jnp.int32)
    product = longitudes[:, None] * orders[None, :] % NLON
    angle = product.astype(jnp.float32) * (2.0 * math.pi / NLON)
    scale = 1.0 / math.sqrt(NLON)
    return jnp.stack([jnp.cos(angle) * scale, -jnp.sin(angle) * scale], axis=1)


def transform(values, table):
    return jnp.einsum("frn,ncm->frcm", values, table, precision=lax.Precision.HIGHEST)


def pack_cycles(masked, plan, slot_dev):
    n_blk = lax.axis_size("blk")
    own_index = lax.axis_index("blk")
    cycle_dev = masked.shape[1]
    cap = (cycle_dev + n_blk - 1) // n_blk
    grid = plan.reshape(n_blk, cycle_dev)
    owner = grid // slot_dev
    positions = jnp.arange(cycle_dev, dtype=jnp.int32)
    earlier = positions[None, :] < positions[:, None]
    same_owner = owner[:, :, None] == owner[:, None, :]
    rank = jnp.sum(same_owner & earlier[None], axis=2, dtype=jnp.int32)
    send_pos = owner * cap + rank
    local_pos = lax.dynamic_index_in_dim(send_pos, own_index, 0, keepdims=False)
    buffer_ids = jnp.arange(n_blk * cap, dtype=jnp.int32)
    send_onehot = (buffer_ids[:, None] == local_pos[None, :]).astype(jnp.float32)
    outgoing = jnp.einsum("qr,frn->fqn", send_onehot, masked, precision=lax.Precision.HIGHEST)
    arrived = lax.all_to_all(outgoing, "blk", split_axis=1, concat_axis=1, tiled=True)
    source_pos = (jnp.arange(n_blk, dtype=jnp.int32)[:, None] * cap + rank).reshape(-1)
    mine = (owner == own_index).reshape(-1)
    slot_local = (grid % slot_dev).reshape(-1)
    slot_ids = jnp.arange(slot_dev, dtype=jnp.int32)
    slot_onehot = ((slot_local[None, :] == slot_ids[:, None]) & mine[None, :]).astype(jnp.float32)
    source_onehot = (source_pos[:, None] == buffer_ids[None, :]).astype(jnp.float32)
    receive_map = jnp.dot(slot_onehot, source_onehot, precision=lax.Precision.HIGHEST)
    return jnp.einsum("pq,fqn->fpn", receive_map, arrived, precision=lax.Precision.HIGHEST)


def degree_sums(legendre, spectrum):
    n_blk = lax.axis_size("blk")
    own_index = lax.axis_index("blk")
    pairs = n_blk // 2
    degree_dev = legendre.shape[2] // n_blk
    own_pair, own_side = own_index // 2, own_index % 2
    swap = [(i, i + 1 - 2 * (i % 2)) for i in range(n_blk)]

    def terms_for(target):
        table = lax.dynamic_slice_in_dim(legendre, target * degree_dev, degree_dev, 2)
        return jnp.einsum("pml,fpcm->lfcm", table, spectrum, preferred_element_type=jnp.float32)

    def pair_sum(step):
        base = (own_pair + step) % pairs * 2
        given = terms_for(base + 1 - own_side).astype(jnp.bfloat16)
        taken = lax.ppermute(given, "blk", swap)
        return terms_for(base + own_side) + taken.astype(jnp.float32)

    steps = sorted(range(1, pairs), key=lambda step: abs(2 * step - pairs))
    arrived = []
    for step in steps:
        shift = [(i, (i + 2 * step) % n_blk) for i in range(n_blk)]
        arrived.append(lax.ppermute(pair_sum(step).astype(jnp.bfloat16), "blk", shift))
    total = pair_sum(0)
    for piece in arrived:
        total = total + piece.astype(jnp.float32)
    return total


def body(field, ocean_mask, plan, legendre):
    lon_local = field.shape[2]
    slot_dev = legendre.shape[0]
    masked = field * ocean_mask.astype(jnp.float32)[None]
    packed = pack_cycles(masked, plan, slot_dev)
    first = lax.axis_index("order") * lon_local
    terms = transform(packed, twiddle(first, lon_local))
    spectrum = lax.psum_scatter(terms, "order", scatter_dimension=3, tiled=True).astype(
        jnp.bfloat16
    )
    coefficients = degree_sums(legendre, spectrum)
    return coefficients


def solution(mesh):
    placed = (P(None, "blk", "order"), P("blk", "order"), P(), P("blk", "order", None))

    def run(field, ocean_mask, plan, legendre):
        chosen = fused_body if fits(mesh, field, legendre) else body
        mapped = jax.shard_map(
            chosen, mesh=mesh, in_specs=placed, out_specs=P("blk", None, None, "order"),
            check_vma=False,
        )
        return mapped(field, ocean_mask, plan, legendre)

    return run
```

```python
import functools
import math

import jax
import jax.numpy as jnp
import numpy as np
from jax import lax
from jax.experimental import pallas as pl
from jax.experimental.pallas import tpu as pltpu
from jax.sharding import PartitionSpec as P

NLON = 4096
M = 1024
MESH = pl.DeviceIdType.MESH
F32, BF16 = jnp.float32, jnp.bfloat16

LINE, PAIR = 4, 2
CHUNK = 2
BASE = 32


def table_of(lon_local, orders):
    coarse = np.arange(lon_local // BASE)[:, None] * BASE
    fine = np.arange(BASE)[:, None]
    m = np.arange(M)[None, :]

    def parts(n, scale):
        angle = (n * m % NLON) * (2.0 * math.pi / NLON)
        return [np.cos(angle) * scale, np.sin(angle) * scale]

    both = parts(coarse, 1.0) + parts(fine, 1.0 / math.sqrt(NLON))
    owners = M // orders
    stacked = np.stack([t.reshape(BASE, owners, orders) for t in both])
    return stacked.transpose(2, 0, 1, 3).astype(np.float32)


def fused_kernel(
    dims,
    field, mask, legendre, table, plan,
    out, far_field,
    leg, spread, own_part, far_part, xs, xr, zr, zbs, zbr, xbs, xbr, wh, wl, near, far, mask_near, mask_far, parts,
    y_own, y_send, y_recv, y_first, y_begun, a_send, a_recv, pick, pack, stage, tabs,
    leg_sem, near_sem, far_sem, mask_sem, tab_sem, out_sem,
    pf_send, pf_recv, pm_send, pm_recv, ys_sem, yr_sem, as_sem, ar_sem,
    xs_sem, xr_sem, zs_sem, zr_sem, zbs_sem, zbr_sem, xbs_sem, xbr_sem, yf_sem, yb_sem,
):
    n, groups, x_groups, tile, m_dev, l_dev, cyc, lon, slot_dev, cap = dims
    m_x = x_groups * tile
    rows = CHUNK * cyc
    n_blk = LINE * PAIR
    b = lax.axis_index("blk")
    o = lax.axis_index("order")
    z, x = b // PAIR, b % PAIR
    side = z // 2
    odd = z % 2
    is_end = 1 - (odd + side - 2 * odd * side)
    far_end = (LINE - 1) * (1 - side)
    far_inner = 2 - side
    mate = 2 * side + 1 - odd
    dest = [
        is_end * far_end + (1 - is_end) * mate,
        is_end * far_inner + (1 - is_end) * far_end,
        is_end * mate + (1 - is_end) * far_inner,
        z,
    ]
    x_peer = b + 1 - 2 * x
    y_peer = (o + 2) % 4
    c_peer = o + 1 - 2 * (o % 2)

    def remote(src, dst, send, recv, blk, order):
        return pltpu.make_async_remote_copy(
            src_ref=src, dst_ref=dst, send_sem=send, recv_sem=recv,
            device_id=(blk, order), device_id_type=MESH,
        )

    def leg_copy(half, j):
        block = dest[j] * PAIR + (x if half == 0 else 1 - x)
        lanes = pl.ds(pl.multiple_of(block * l_dev, l_dev), l_dev)
        return pltpu.make_async_copy(
            legendre.at[:, :, lanes],
            leg.at[half, :, :, pl.ds(j * l_dev, l_dev)],
            leg_sem.at[half, j],
        )

    def near_copy(h):
        return pltpu.make_async_copy(
            field.at[pl.ds(h * CHUNK, CHUNK)], near.at[h % 2], near_sem.at[h % 2]
        )

    def far_copy(h):
        return pltpu.make_async_copy(
            far_field.at[pl.ds(h * CHUNK, CHUNK)], far.at[h % 2], far_sem.at[h % 2]
        )

    def push_field(h):
        fields = pl.ds(h * CHUNK, CHUNK)
        return remote(
            field.at[fields], far_field.at[fields], pf_send.at[h], pf_recv.at[h], b, c_peer
        )

    def push_first(h):
        return remote(
            near.at[h], far.at[h], pf_send.at[h], pf_recv.at[h], b, c_peer
        )

    tab_own = pltpu.make_async_copy(table.at[o], tabs.at[0], tab_sem.at[0])
    tab_other = pltpu.make_async_copy(table.at[y_peer], tabs.at[1], tab_sem.at[1])
    tab_own.start()
    tab_other.start()
    mask_own = pltpu.make_async_copy(mask, mask_near, mask_sem)
    mask_own.start()
    near_copy(0).start()
    near_copy(1).start()

    barrier = pltpu.get_barrier_semaphore()
    for k in range(1, n_blk):
        pl.semaphore_signal(barrier, inc=1, device_id=((b + k) % n_blk, o), device_id_type=MESH)
    pl.semaphore_signal(barrier, inc=1, device_id=(b, y_peer), device_id_type=MESH)
    pl.semaphore_signal(barrier, inc=1, device_id=(b, c_peer), device_id_type=MESH)

    def iota(shape, axis):
        return lax.broadcasted_iota(jnp.int32, shape, axis)

    wanted = (b * slot_dev + iota((1, slot_dev * tile), 1) // tile).astype(F32)
    row_id, col_id = iota((cyc, cyc), 0), iota((cyc, cyc), 1)
    send_at = jnp.zeros((1, cyc), F32)
    source = jnp.zeros((cyc, slot_dev * tile), F32)
    for block in range(n_blk):
        across = plan[:, pl.ds(block * cyc, cyc)].astype(F32)
        down = jnp.sum(jnp.where(row_id == col_id, across, 0.0), axis=1, keepdims=True)
        owner_across = jnp.floor((across + 0.5) * (1.0 / slot_dev))
        owner_down = jnp.floor((down + 0.5) * (1.0 / slot_dev))
        same = owner_down == owner_across
        rank_across = jnp.sum(
            jnp.where(same & (row_id < col_id), 1.0, 0.0), axis=0, keepdims=True
        )
        rank_down = jnp.sum(
            jnp.where(same & (col_id < row_id), 1.0, 0.0), axis=1, keepdims=True
        )
        here = jnp.where(b == block, 1.0, 0.0)
        send_at += here * (owner_across * cap + rank_across)
        source += jnp.where(down == wanted, block * cap + rank_down, 0.0)
    source = jnp.sum(source, axis=0, keepdims=True)
    per = CHUNK * cap
    r = iota((rows, cyc), 0)
    position = (r // per * cap + r % cap).astype(F32)
    for f in range(CHUNK):
        hit = (position == send_at) & (r % per // cap == f)
        pack[:, pl.ds(f * cyc, cyc)] = jnp.where(hit, 1.0, 0.0).astype(BF16)
    r = iota((rows, slot_dev * tile), 0)
    position = (r // per * cap + r % cap).astype(F32)
    for f in range(CHUNK):
        hit = (position == source) & (r % per // cap == f)
        pick[f] = jnp.where(hit, 1.0, 0.0).astype(BF16)

    pl.semaphore_wait(barrier, n_blk + 1)

    push_mask = remote(mask_near, mask_far, pm_send, pm_recv, b, c_peer)
    mask_own.wait()
    push_mask.start()
    for h in range(2):
        near_copy(h).wait()
        push_first(h).start()

    @pl.loop(2, n)
    def _(h):
        push_field(h).start()

    tab_own.wait()
    tab_other.wait()
    for side_of in range(2):

        @pl.loop(0, lon // BASE)
        def _(a):
            ca = tabs[side_of, 0, pl.ds(a, 1), :]
            sa = tabs[side_of, 1, pl.ds(a, 1), :]
            cb = tabs[side_of, 2]
            sb = tabs[side_of, 3]
            at = pl.ds(pl.multiple_of(a * BASE, BASE), BASE)
            for c, value in enumerate((ca * cb - sa * sb, -(sa * cb + ca * sb))):
                high = value.astype(BF16)
                wh[side_of, at, pl.ds(c * m_dev, m_dev)] = high
                rest = value - high.astype(F32)
                wl[side_of, at, pl.ds(c * m_dev, m_dev)] = rest.astype(BF16)

    push_mask.wait()

    def turn(index):
        quarter = (index * iota((1, m_dev), 1)) % 4
        real = jnp.where(quarter == 0, 1.0, jnp.where(quarter == 2, -1.0, 0.0))
        imag = jnp.where(quarter == 3, 1.0, jnp.where(quarter == 1, -1.0, 0.0))
        return real, imag

    def y_copy(h):
        return remote(y_send.at[h % 2], y_recv.at[h], ys_sem.at[h % 2], yr_sem.at[h % 4], b, y_peer)

    first_y = remote(y_first, y_begun, yf_sem, yb_sem, b, y_peer)

    def transform(h):
        @pl.when(h < 2)
        def _():
            push_first(h).wait()

        @pl.when(h == 0)
        def _():
            for j in range(LINE):
                leg_copy(1, j).start()

        @pl.when(h >= 2)
        def _():
            near_copy(h).wait()
            far_copy(h).wait()

        @pl.when((h >= 1) & (h + 1 < n))
        def _():
            near_copy(h + 1).start()
            push_field(h + 1).wait()
            far_copy(h + 1).start()

        @pl.when(h == 1)
        def _():
            for j in range(LINE):
                leg_copy(0, j).start()

        @pl.when(h >= 3)
        def _():
            y_copy(h - 2).wait_send()

        for i, (data, wet) in enumerate(((near, mask_near), (far, mask_far))):
            value = (data[h % 2] * wet[...].astype(F32)[None]).reshape(rows, lon)
            high = value.astype(BF16)
            parts[pl.ds(i * rows, rows), :] = high
            rest = value - high.astype(F32)
            parts[pl.ds((2 + i) * rows, rows), :] = rest.astype(BF16)
        near_r, near_i = turn(o)
        far_r, far_i = turn(c_peer)
        for side_of in (1, 0):
            both = jnp.dot(parts[...], wh[side_of], preferred_element_type=F32)
            total = both[: 2 * rows] + both[2 * rows :]
            total += jnp.dot(
                parts[pl.ds(0, 2 * rows), :], wl[side_of], preferred_element_type=F32
            )
            nr, ni = total[:rows, :m_dev], total[:rows, m_dev:]
            fr, fi = total[rows:, :m_dev], total[rows:, m_dev:]
            real = near_r * nr - near_i * ni + far_r * fr - far_i * fi
            imag = near_r * ni + near_i * nr + far_r * fi + far_i * fr
            if side_of:

                @pl.when(h == 0)
                def _():
                    y_first[:, pl.ds(0, m_dev)] = real.astype(BF16)
                    y_first[:, pl.ds(m_dev, m_dev)] = imag.astype(BF16)
                    first_y.start()

                @pl.when(h > 0)
                def _():
                    y_send[h % 2, :, pl.ds(0, m_dev)] = real
                    y_send[h % 2, :, pl.ds(m_dev, m_dev)] = imag
                    y_copy(h).start()

            else:
                y_own[h % 2, :, pl.ds(0, m_dev)] = real
                y_own[h % 2, :, pl.ds(m_dev, m_dev)] = imag

    def a_copy(h, k):
        to = (b + k) % n_blk
        return remote(
            a_send.at[h, to], a_recv.at[h, b], as_sem.at[h % 4, k - 1], ar_sem.at[h % 4, k - 1], to, o
        )

    def exchange(h):
        @pl.when(h == 0)
        def _():
            first_y.wait()
            y_recv[h] = y_begun[...].astype(F32)

        @pl.when(h > 0)
        def _():
            y_copy(h).wait_recv()

        spectrum = (y_own[h % 2] + y_recv[h]).astype(BF16)
        packed = jnp.dot(pack[...], spectrum, preferred_element_type=F32).astype(BF16)
        a_send[h] = packed.reshape(n_blk, per, 2 * m_dev)
        a_recv[h, b] = a_send[h, b]
        for k in range(1, n_blk):
            a_copy(h, k).start()

    diagonal = (iota((1, tile, slot_dev * tile), 1)) == (iota((1, tile, slot_dev * tile), 2) % tile)

    def spread_out(h):
        for k in range(1, n_blk):
            a_copy(h, k).wait()
        got = a_recv[h].reshape(rows, 2 * m_dev)
        for c in range(2):
            for f in range(CHUNK):
                value = lax.dot_general(
                    got[:, c * m_dev : (c + 1) * m_dev], pick[f],
                    (((0,), (0,)), ((), ())), preferred_element_type=F32,
                )
                value = value.reshape(groups, tile, slot_dev * tile)
                spread[:, pl.ds((f * 2 + c) * tile, tile), :] = jnp.where(
                    diagonal, value, 0.0
                ).astype(BF16)

    def x_copy(h, j):
        return remote(
            xs.at[h % 2, j], xr.at[h % 5, j], xs_sem.at[h % 2, j], xr_sem.at[h % 5, j], x_peer, o
        )

    def product(g, half, first=0, count=LINE):
        at = pl.ds(pl.multiple_of(g * tile, tile), tile)
        lanes = pl.ds(first * l_dev, count * l_dev)
        table_part = leg[half, :, at, lanes].reshape(slot_dev * tile, count * l_dev)
        return at, jnp.dot(spread[g], table_part, preferred_element_type=F32)

    def low_end_copy(h):
        return remote(
            zbs.at[h], zbr.at[h, pl.ds(0, LINE - 1)], zbs_sem.at[h % 4, 0], zbr_sem.at[h % 4, 0],
            mate * PAIR + x, o,
        )

    def low_inner_copy(h, j):
        to_z = (mate, far_end, far_inner)[j]
        return remote(
            zbs.at[h, j], zbr.at[h, (0, 1, 3)[j]], zbs_sem.at[h % 4, j],
            zbr_sem.at[h % 4, (0, 1, 1)[j]], to_z * PAIR + x, o,
        )

    def low_x_copy(h):
        return remote(xbs.at[h], xbr.at[h], xbs_sem.at[h % 4], xbr_sem.at[h % 4], x_peer, o)

    def low_part(h, j, half):
        if half == 0:
            return own_part[h % 3, j, :, pl.ds(m_x, m_dev - m_x), :]
        return far_part[h % 3, j]

    def low_middle(h):
        @pl.when(is_end == 0)
        def _():
            low_end_copy(h).wait_recv()
            for j in (1, 2):
                for half in range(2):
                    value = low_part(h, j, half) + zbr[h, j - 1, half].astype(F32)
                    zbs[h, j, half] = value.astype(BF16)
                low_inner_copy(h, j).start()

    def low_across(h):
        def add(first, second):
            for half in (1, 0):
                value = low_part(h, LINE - 1, half)
                value += zbr[h, first, half].astype(F32) + zbr[h, second, half].astype(F32)
                if half == 0:
                    own_part[h % 3, LINE - 1, :, pl.ds(m_x, m_dev - m_x), :] = value
                else:
                    xbs[h] = value.astype(BF16)
            low_x_copy(h).start()

        @pl.when(is_end == 1)
        def _():
            low_inner_copy(h, 0).wait_recv()
            low_inner_copy(h, 1).wait_recv()
            add(0, 1)

        @pl.when(is_end == 0)
        def _():
            low_inner_copy(h, 2).wait_recv()
            add(2, 3)

    def products(h):
        @pl.when(h == 0)
        def _():
            for j in range(LINE):
                leg_copy(1, j).wait()

        @pl.when(h >= 2)
        def _():
            for j in range(LINE):
                x_copy(h - 2, j).wait_send()

        def x_products(first, count):
            @pl.loop(0, x_groups)
            def _(g):
                at, value = product(g, 1, first, count)
                for j in range(count):
                    piece = value[:, j * l_dev : (j + 1) * l_dev].reshape(2 * CHUNK, tile, l_dev)
                    xs[h % 2, first + j, :, at, :] = piece.astype(BF16)

        def x_start(first, count):
            for j in range(count):
                x_copy(h, first + j).start()

        @pl.when(h == 0)
        def _():
            x_products(0, 2)
            exchange(1)
            x_start(0, 2)
            x_products(2, 2)
            x_start(2, 2)

        @pl.when(h > 0)
        def _():
            x_products(0, LINE)
            x_start(0, LINE - 1)

            @pl.when(h < n - 1)
            def _():
                x_start(LINE - 1, 1)

        @pl.when(h == 0)
        def _():
            for j in range(LINE):
                leg_copy(0, j).wait()

        @pl.loop(x_groups, groups)
        def _(g):
            low = pl.ds(pl.multiple_of((g - x_groups) * tile, tile), tile)
            for half in range(2):
                at, value = product(g, half)
                for j in range(LINE):
                    piece = value[:, j * l_dev : (j + 1) * l_dev].reshape(2 * CHUNK, tile, l_dev)
                    if half == 0:
                        own_part[h % 3, j, :, at, :] = piece
                    else:
                        far_part[h % 3, j, :, low, :] = piece
                    if j < LINE - 1:
                        zbs[h, j, half, :, low, :] = piece.astype(BF16)

        @pl.when(is_end == 1)
        def _():
            low_end_copy(h).start()

        @pl.when(is_end == 0)
        def _():
            low_inner_copy(h, 0).start()

        @pl.loop(0, x_groups)
        def _(g):
            at, value = product(g, 0)
            for j in range(LINE):
                piece = value[:, j * l_dev : (j + 1) * l_dev].reshape(2 * CHUNK, tile, l_dev)
                own_part[h % 3, j, :, at, :] = piece

    def z_copy(h, j, to_z, slot):
        return remote(
            xr.at[h % 5, j], zr.at[h % 4, slot], zs_sem.at[h % 4, j], zr_sem.at[h % 4, slot],
            to_z * PAIR + x, o,
        )

    def end_copy(h, j):
        return z_copy(h, j, mate, j)

    def inner_copy(h, j):
        return z_copy(h, j, (mate, far_end, far_inner)[j], (0, 1, 3)[j])

    high = pl.ds(0, m_x)

    def first_sums(h):
        for j in range(LINE):
            if j == LINE - 1:

                @pl.when(h == n - 1)
                def _():
                    low_across(h)
                    last_sums(h - 1)

            x_copy(h, j).wait_recv()
            value = own_part[h % 3, j, :, high, :] + xr[h % 5, j].astype(F32)
            if j == LINE - 1:
                own_part[h % 3, j, :, high, :] = value
                continue

            @pl.when(is_end == 1)
            def _():
                xr[h % 5, j] = value.astype(BF16)
                end_copy(h, j).start()

            @pl.when(is_end == 0)
            def _():
                if j == 0:
                    xr[h % 5, j] = value.astype(BF16)
                else:
                    end_copy(h, j - 1).wait_recv()
                    xr[h % 5, j] = (value + zr[h % 4, j - 1].astype(F32)).astype(BF16)
                inner_copy(h, j).start()

    def out_copy(h):
        return pltpu.make_async_copy(
            stage.at[h % 2], out.at[:, pl.ds(h * CHUNK, CHUNK)], out_sem.at[h % 2]
        )

    def last_sums(h):
        @pl.when(h >= 2)
        def _():
            out_copy(h - 2).wait()

        def add(first, second):
            value = own_part[h % 3, LINE - 1, :, high, :]
            value += zr[h % 4, first].astype(F32) + zr[h % 4, second].astype(F32)
            own_part[h % 3, LINE - 1, :, high, :] = value

        @pl.when(is_end == 1)
        def _():
            inner_copy(h, 0).wait_recv()
            inner_copy(h, 1).wait_recv()
            add(0, 1)
            for j in range(LINE - 1):
                end_copy(h, j).wait_send()
            low_end_copy(h).wait_send()

        @pl.when(is_end == 0)
        def _():
            end_copy(h, 2).wait_recv()
            inner_copy(h, 2).wait_recv()
            add(2, 3)
            for j in range(LINE - 1):
                inner_copy(h, j).wait_send()
                low_inner_copy(h, j).wait_send()

        low_x_copy(h).wait_recv()
        low = pl.ds(m_x, m_dev - m_x)
        own_part[h % 3, LINE - 1, :, low, :] += xbr[h].astype(F32)
        for f in range(CHUNK):
            for c in range(2):
                stage[h % 2, :, f, c, :] = own_part[h % 3, LINE - 1, 2 * f + c].T
        low_x_copy(h).wait_send()
        out_copy(h).start()

    @pl.loop(0, n + 5)
    def _(t):
        def when(step, delay):
            @pl.when((t >= delay) & (t < n + delay))
            def _():
                step(t - delay)

        @pl.when((t >= 5) & (t != n + 3) & (t < n + 5))
        def _():
            last_sums(t - 5)


        @pl.when((t >= 4) & (t < n + 3))
        def _():
            low_across(t - 4)

        @pl.when(t == n + 2)
        def _():
            x_copy(n - 1, LINE - 1).start()

        when(transform, 0)

        @pl.when((t >= 1) & (t != 2) & (t < n + 1))
        def _():
            exchange(t - 1)

        when(spread_out, 2)
        when(products, 2)
        when(low_middle, 3)
        when(first_sums, 3)

    for h in (n - 2, n - 1):
        y_copy(h).wait_send()
        out_copy(h).wait()
        for j in range(LINE):
            x_copy(h, j).wait_send()


def fused_body(field, ocean_mask, plan, legendre):
    fields, cyc, lon = field.shape
    slot_dev, m_dev, degrees = legendre.shape
    n_blk = LINE * PAIR
    l_dev = degrees // n_blk
    tile = 16
    groups = m_dev // tile
    n = fields // CHUNK
    rows = CHUNK * cyc
    cap = (cyc + n_blk - 1) // n_blk
    per = CHUNK * cap
    table = jnp.asarray(table_of(lon, m_dev))
    x_groups = groups - max(groups // 8, 1)
    piece = (2 * CHUNK, m_dev, l_dev)
    high = (2 * CHUNK, x_groups * tile, l_dev)
    low = (2 * CHUNK, m_dev - x_groups * tile, l_dev)
    dma = pltpu.SemaphoreType.DMA
    any_spec = pl.BlockSpec(memory_space=pl.ANY)
    vmem_spec = pl.BlockSpec(memory_space=pltpu.VMEM)
    scratch = [
        pltpu.VMEM((2, slot_dev, m_dev, LINE * l_dev), BF16),
        pltpu.VMEM((groups, 2 * CHUNK * tile, slot_dev * tile), BF16),
        pltpu.VMEM((3, LINE) + piece, F32),
        pltpu.VMEM((3, LINE) + low, F32),
        pltpu.VMEM((2, LINE) + high, BF16),
        pltpu.VMEM((5, LINE) + high, BF16),
        pltpu.VMEM((4, 4) + high, BF16),
        pltpu.VMEM((n, LINE - 1, 2) + low, BF16),
        pltpu.VMEM((n, 4, 2) + low, BF16),
        pltpu.VMEM((n,) + low, BF16),
        pltpu.VMEM((n,) + low, BF16),
        pltpu.VMEM((2, lon, 2 * m_dev), BF16),
        pltpu.VMEM((2, lon, 2 * m_dev), BF16),
        pltpu.VMEM((2, CHUNK, cyc, lon), F32),
        pltpu.VMEM((2, CHUNK, cyc, lon), F32),
        pltpu.VMEM((cyc, lon), jnp.int32),
        pltpu.VMEM((cyc, lon), jnp.int32),
        pltpu.VMEM((4 * rows, lon), BF16),
        pltpu.VMEM((2, rows, 2 * m_dev), F32),
        pltpu.VMEM((2, rows, 2 * m_dev), F32),
        pltpu.VMEM((n, rows, 2 * m_dev), F32),
        pltpu.VMEM((rows, 2 * m_dev), BF16),
        pltpu.VMEM((rows, 2 * m_dev), BF16),
        pltpu.VMEM((n, n_blk, per, 2 * m_dev), BF16),
        pltpu.VMEM((n, n_blk, per, 2 * m_dev), BF16),
        pltpu.VMEM((CHUNK, rows, slot_dev * tile), BF16),
        pltpu.VMEM((rows, rows), BF16),
        pltpu.VMEM((2, l_dev, CHUNK, 2, m_dev), F32),
        pltpu.VMEM((2, 4, BASE, m_dev), F32),
        dma((2, LINE)),
        dma((2,)),
        dma((2,)),
        dma,
        dma((2,)),
        dma((2,)),
        dma((n,)), dma((n,)),
        dma, dma,
        dma((2,)), dma((4,)),
        dma((4, n_blk - 1)), dma((4, n_blk - 1)),
        dma((2, LINE)), dma((5, LINE)),
        dma((4, 3)), dma((4, 4)),
        dma((4, 3)), dma((4, 2)),
        dma((4,)), dma((4,)),
        dma, dma,
    ]
    dims = (n, groups, x_groups, tile, m_dev, l_dev, cyc, lon, slot_dev, cap)
    sums, _ = pl.pallas_call(
        functools.partial(fused_kernel, dims),
        out_shape=[
            jax.ShapeDtypeStruct((l_dev, fields, 2, m_dev), F32),
            jax.ShapeDtypeStruct(field.shape, F32),
        ],
        in_specs=[any_spec] * 4 + [vmem_spec],
        out_specs=[any_spec] * 2,
        scratch_shapes=scratch,
        compiler_params=pltpu.CompilerParams(
            collective_id=0, has_side_effects=True, vmem_limit_bytes=66 * 1000 * 1000
        ),
        name="analysis",
    )(field, ocean_mask, legendre, table, plan.reshape(1, -1))
    parts = 8
    return pl.pallas_call(
        hand_on_kernel,
        out_shape=jax.ShapeDtypeStruct(sums.shape, F32),
        in_specs=[any_spec],
        out_specs=any_spec,
        scratch_shapes=[
            pltpu.VMEM((parts, l_dev // parts) + sums.shape[1:], F32),
            dma((parts,)), dma((parts,)),
        ],
        name="hand_on",
    )(sums)


def hand_on_kernel(source, target, held, in_sem, out_sem):
    parts, depth = held.shape[:2]

    def into(k):
        return pltpu.make_async_copy(source.at[pl.ds(k * depth, depth)], held.at[k], in_sem.at[k])

    def away(k):
        return pltpu.make_async_copy(held.at[k], target.at[pl.ds(k * depth, depth)], out_sem.at[k])

    for k in range(parts):
        into(k).start()
    for k in range(parts):
        into(k).wait()
        away(k).start()
    for k in range(parts):
        away(k).wait()


def fits(mesh, field, legendre):
    shape = dict(mesh.shape)
    n_blk, n_order = shape["blk"], shape["order"]
    cyc, lon = field.shape[1] // n_blk, field.shape[2] // n_order
    slots, m_dev = legendre.shape[0] // n_blk, legendre.shape[1] // n_order
    return (
        n_blk == LINE * PAIR
        and n_order == 4
        and field.shape[0] % CHUNK == 0
        and field.shape[0] // CHUNK >= 5
        and lon == BASE * BASE
        and NLON == 4 * lon
        and m_dev % 128 == 0
        and legendre.shape[2] == n_blk * 128
        and cyc % n_blk == 0
        and slots % 8 == 0
    )


def twiddle(first, count):
    longitudes = first + jnp.arange(count, dtype=jnp.int32)
    orders = jnp.arange(M, dtype=jnp.int32)
    product = longitudes[:, None] * orders[None, :] % NLON
    angle = product.astype(jnp.float32) * (2.0 * math.pi / NLON)
    scale = 1.0 / math.sqrt(NLON)
    return jnp.stack([jnp.cos(angle) * scale, -jnp.sin(angle) * scale], axis=1)


def transform(values, table):
    return jnp.einsum("frn,ncm->frcm", values, table, precision=lax.Precision.HIGHEST)


def pack_cycles(masked, plan, slot_dev):
    n_blk = lax.axis_size("blk")
    own_index = lax.axis_index("blk")
    cycle_dev = masked.shape[1]
    cap = (cycle_dev + n_blk - 1) // n_blk
    grid = plan.reshape(n_blk, cycle_dev)
    owner = grid // slot_dev
    positions = jnp.arange(cycle_dev, dtype=jnp.int32)
    earlier = positions[None, :] < positions[:, None]
    same_owner = owner[:, :, None] == owner[:, None, :]
    rank = jnp.sum(same_owner & earlier[None], axis=2, dtype=jnp.int32)
    send_pos = owner * cap + rank
    local_pos = lax.dynamic_index_in_dim(send_pos, own_index, 0, keepdims=False)
    buffer_ids = jnp.arange(n_blk * cap, dtype=jnp.int32)
    send_onehot = (buffer_ids[:, None] == local_pos[None, :]).astype(jnp.float32)
    outgoing = jnp.einsum("qr,frn->fqn", send_onehot, masked, precision=lax.Precision.HIGHEST)
    arrived = lax.all_to_all(outgoing, "blk", split_axis=1, concat_axis=1, tiled=True)
    source_pos = (jnp.arange(n_blk, dtype=jnp.int32)[:, None] * cap + rank).reshape(-1)
    mine = (owner == own_index).reshape(-1)
    slot_local = (grid % slot_dev).reshape(-1)
    slot_ids = jnp.arange(slot_dev, dtype=jnp.int32)
    slot_onehot = ((slot_local[None, :] == slot_ids[:, None]) & mine[None, :]).astype(jnp.float32)
    source_onehot = (source_pos[:, None] == buffer_ids[None, :]).astype(jnp.float32)
    receive_map = jnp.dot(slot_onehot, source_onehot, precision=lax.Precision.HIGHEST)
    return jnp.einsum("pq,fqn->fpn", receive_map, arrived, precision=lax.Precision.HIGHEST)


def degree_sums(legendre, spectrum):
    n_blk = lax.axis_size("blk")
    own_index = lax.axis_index("blk")
    pairs = n_blk // 2
    degree_dev = legendre.shape[2] // n_blk
    own_pair, own_side = own_index // 2, own_index % 2
    swap = [(i, i + 1 - 2 * (i % 2)) for i in range(n_blk)]

    def terms_for(target):
        table = lax.dynamic_slice_in_dim(legendre, target * degree_dev, degree_dev, 2)
        return jnp.einsum("pml,fpcm->lfcm", table, spectrum, preferred_element_type=jnp.float32)

    def pair_sum(step):
        base = (own_pair + step) % pairs * 2
        given = terms_for(base + 1 - own_side).astype(jnp.bfloat16)
        taken = lax.ppermute(given, "blk", swap)
        return terms_for(base + own_side) + taken.astype(jnp.float32)

    steps = sorted(range(1, pairs), key=lambda step: abs(2 * step - pairs))
    arrived = []
    for step in steps:
        shift = [(i, (i + 2 * step) % n_blk) for i in range(n_blk)]
        arrived.append(lax.ppermute(pair_sum(step).astype(jnp.bfloat16), "blk", shift))
    total = pair_sum(0)
    for piece in arrived:
        total = total + piece.astype(jnp.float32)
    return total


def body(field, ocean_mask, plan, legendre):
    lon_local = field.shape[2]
    slot_dev = legendre.shape[0]
    masked = field * ocean_mask.astype(jnp.float32)[None]
    packed = pack_cycles(masked, plan, slot_dev)
    first = lax.axis_index("order") * lon_local
    terms = transform(packed, twiddle(first, lon_local))
    spectrum = lax.psum_scatter(terms, "order", scatter_dimension=3, tiled=True).astype(
        jnp.bfloat16
    )
    coefficients = degree_sums(legendre, spectrum)
    return coefficients


def solution(mesh):
    placed = (P(None, "blk", "order"), P("blk", "order"), P(), P("blk", "order", None))

    def run(field, ocean_mask, plan, legendre):
        chosen = fused_body if fits(mesh, field, legendre) else body
        mapped = jax.shard_map(
            chosen, mesh=mesh, in_specs=placed, out_specs=P("blk", None, None, "order"),
            check_vma=False,
        )
        return mapped(field, ocean_mask, plan, legendre)

    return run
```
